64 devices in a mesh: data: 4 (over x, y), seq: 16 (over z, core).
Axes of the slice: x: 2, y: 2, z: 8, core: 2. Of those that a mesh axis runs over, the one named last changes fastest.
The devices are a block of a 4x4x8 slice.
Arguments:
- tokens: bfloat16 [32, 16384, 384], P('data', 'seq'), parts along dimension 0
- lengths: int32 [32], P('data'), parts along dimension 0
- slot_params: bfloat16 [384, 256], replicated
- logit_scale: float32 [1], replicated
- w_in: bfloat16 [128, 384, 1536], P('seq')
- w_out: bfloat16 [128, 1536, 384], P('seq')
Outputs:
- output: bfloat16 [32, 16384, 384], P('data', 'seq'), parts along dimension 0
There are 4 independent parts. The reference program is written for one: setup_inputs(seed, part) draws one part's arguments, and reference() takes and returns one part's arrays. A program takes and returns all parts, laid end to end along the dimension named above; an argument that names none is the same for every part.
All inputs are finite; a program needn't handle non-finite values.
Results may differ from the reference program's by a relative error of at most 0.0173106.
Values are sent between devices in bfloat16 or wider.
A program may use at most 768 MiB of HBM per device.

```python
import jax
import jax.numpy as jnp
from jax import lax

BATCH = 8
TOKENS = 16384
D_MODEL = 384
FF_DIM = 1536
EXPERTS = 128
SLOTS = 2
NUM_SLOTS = EXPERTS * SLOTS


def setup_inputs(seed: int = 0, part: int = 0) -> dict:
    base_key = jax.random.key(seed)
    k_phi, k_win, k_wout, k_gain = jax.random.split(base_key, 4)
    part_key = jax.random.fold_in(base_key, part)
    k_sel, k_noise, k_len = jax.random.split(part_key, 3)
    slot_params = jax.random.normal(k_phi, (D_MODEL, NUM_SLOTS), jnp.float32)
    chosen = jax.random.randint(k_sel, (BATCH, TOKENS), 0, NUM_SLOTS)
    noise = jax.random.normal(k_noise, (BATCH, TOKENS, D_MODEL), jnp.float32)
    tokens = jnp.take(slot_params.T, chosen, axis=0) + noise
    lengths = jax.random.randint(k_len, (BATCH,), 1, TOKENS + 1)
    logit_scale = jax.random.uniform(k_gain, (1,), jnp.float32, 6.0, 9.0)
    w_in = jax.random.normal(k_win, (EXPERTS, D_MODEL, FF_DIM), jnp.float32) * D_MODEL ** -0.5
    w_out = jax.random.normal(k_wout, (EXPERTS, FF_DIM, D_MODEL), jnp.float32) * FF_DIM ** -0.5
    return {
        "tokens": tokens.astype(jnp.bfloat16),
        "lengths": lengths.astype(jnp.int32),
        "slot_params": slot_params.astype(jnp.bfloat16),
        "logit_scale": logit_scale,
        "w_in": w_in.astype(jnp.bfloat16),
        "w_out": w_out.astype(jnp.bfloat16),
    }


def reference(tokens, lengths, slot_params, logit_scale, w_in, w_out):
    params_f32 = slot_params.astype(jnp.float32)
    col_inv = lax.rsqrt(jnp.sum(params_f32 * params_f32, axis=0, keepdims=True) + 1e-6)
    phi_norm = (params_f32 * (logit_scale[0] * col_inv)).astype(jnp.bfloat16)
    positions = jnp.arange(TOKENS)

    def row_logits(row_tokens):
        tok_f32 = row_tokens.astype(jnp.float32)
        tok_norm = (tok_f32 * lax.rsqrt(jnp.sum(tok_f32 * tok_f32, axis=-1, keepdims=True) + 1e-6)).astype(jnp.bfloat16)
        return jnp.dot(tok_norm, phi_norm, preferred_element_type=jnp.float32)

    def dispatch_row(row_args):
        row_tokens, row_len = row_args
        logits = row_logits(row_tokens)
        is_valid = (positions < row_len)[:, None]
        col_max = jnp.max(jnp.where(is_valid, logits, -jnp.inf), axis=0)
        disp_w = jnp.where(is_valid, jnp.exp(logits - col_max[None, :]), 0.0)
        col_sum = jnp.sum(disp_w, axis=0)
        slot_sum = jnp.dot(disp_w.astype(jnp.bfloat16).T, row_tokens, preferred_element_type=jnp.float32)
        return (slot_sum / col_sum[:, None]).astype(jnp.bfloat16)

    slot_in = lax.map(dispatch_row, (tokens, lengths))
    by_expert = slot_in.reshape(BATCH, EXPERTS, SLOTS, D_MODEL).transpose(1, 0, 2, 3).reshape(EXPERTS, BATCH * SLOTS, D_MODEL)

    def expert_ffn(exp_args):
        exp_in, exp_w_in, exp_w_out = exp_args
        hidden = jax.nn.gelu(jnp.dot(exp_in, exp_w_in, preferred_element_type=jnp.float32)).astype(jnp.bfloat16)
        return jnp.dot(hidden, exp_w_out, preferred_element_type=jnp.float32).astype(jnp.bfloat16)

    expert_out = lax.map(expert_ffn, (by_expert, w_in, w_out))
    slot_out = expert_out.reshape(EXPERTS, BATCH, SLOTS, D_MODEL).transpose(1, 0, 2, 3).reshape(BATCH, NUM_SLOTS, D_MODEL)

    def combine_row(row_args):
        row_tokens, row_len, row_slots = row_args
        logits = row_logits(row_tokens)
        is_valid = (positions < row_len)[:, None]
        combine_w = jax.nn.softmax(logits, axis=-1).astype(jnp.bfloat16)
        mixed = jnp.dot(combine_w, row_slots, preferred_element_type=jnp.float32).astype(jnp.bfloat16)
        return jnp.where(is_valid, mixed, jnp.zeros_like(mixed))

    return lax.map(combine_row, (tokens, lengths, slot_out))
```

```python
import functools

import jax
import jax.numpy as jnp
from jax import lax
from jax.experimental import pallas as pl
from jax.experimental.pallas import tpu as pltpu
from jax.sharding import PartitionSpec as P

F32 = jnp.float32
BF16 = jnp.bfloat16
MESH = pl.DeviceIdType.MESH
NT = (((1,), (1,)), ((), ()))
UP, DOWN = 0, 1
GROUP_ROWS = 2
HALVES = 2
CORES = 2


def _exchange_kernel(dims, len_ref, scale_ref, phi_ref, tok_ref, win_ref, wout_ref, comb_ref, gat_ref,
                     xbuf, xnbuf, phi_ring, phi_comb, part, pin, chip, sbuf, rbuf, zpart, zpin, zchip, zrecv,
                     slot_in, win, wout, gath, ypart, cbuf,
                     x_sem, win_sem, wout_sem, pr_send, pr_recv, rs_send, rs_recv, z_send, z_recv,
                     ag_send, ag_recv, pg_send, pg_recv, lg_sem, c_sem):
    rows, toks, width, slots, seq, experts, ff = dims
    chips = seq // CORES
    own = slots // seq
    per = own // experts
    groups = rows // GROUP_ROWS
    far = chips // 2
    half_e = experts // HALVES
    hs = own // HALVES
    par = slots // CORES

    me = lax.axis_index("seq")
    z = me // CORES
    core = me % CORES
    other = 1 - core

    def chip_at(delta):
        return (z + delta + chips) % chips

    def dev_at(delta):
        return chip_at(delta) * CORES + core

    partner = z * CORES + other
    up, down = dev_at(1), dev_at(-1)
    target = {UP: up, DOWN: down}

    barrier = pltpu.get_barrier_semaphore()
    for delta in range(1, chips):
        pl.semaphore_signal(barrier, inc=1, device_id={"seq": dev_at(delta)}, device_id_type=MESH)
    pl.semaphore_signal(barrier, inc=1, device_id={"seq": partner}, device_id_type=MESH)

    x_copies = [pltpu.make_async_copy(tok_ref.at[b], xbuf.at[b], x_sem.at[b]) for b in range(rows)]
    for copy in x_copies:
        copy.start()
    w_copies = []
    for h in range(HALVES):
        es = pl.ds(h * half_e, half_e)
        w_copies.append((pltpu.make_async_copy(win_ref.at[es], win.at[es], win_sem.at[h]),
                         pltpu.make_async_copy(wout_ref.at[es], wout.at[es], wout_sem.at[h])))
    for pair in w_copies:
        for copy in pair:
            copy.start()

    gain = scale_ref[0]
    params = phi_ref[...].astype(F32)
    col_inv = lax.rsqrt(jnp.sum(params * params, axis=0, keepdims=True) + 1e-6)
    phi_norm = (params * (gain * col_inv)).astype(BF16).astype(F32)
    phi_t = phi_norm.T
    ring_order = [phi_t[(d * CORES + p) * own:(d * CORES + p + 1) * own] for p in range(CORES) for d in range(chips)]
    phi_ring[...] = jnp.concatenate(ring_order, axis=0).astype(BF16)
    comb_order = [phi_t[i * own + h * hs:i * own + (h + 1) * hs] for h in range(HALVES) for i in range(seq)]
    phi_comb[...] = jnp.concatenate(comb_order, axis=0).astype(BF16)
    bound = gain * 1.01
    zlane = lax.broadcasted_iota(jnp.int32, (slots, 128), 1)
    zpart[...] = jnp.zeros_like(zpart)

    def dispatch_row(b, carry):
        x = xbuf[b]
        xf = x.astype(F32)
        inv = lax.rsqrt(jnp.sum(xf * xf, axis=-1, keepdims=True) + 1e-6)
        xn = (xf * inv).astype(BF16)
        xnbuf[b] = xn
        lt = lax.dot_general(phi_ring[...], xn, NT, preferred_element_type=F32)
        pos = me * toks + lax.broadcasted_iota(jnp.int32, (1, toks), 1)
        w = jnp.where(pos < len_ref[b], jnp.exp(lt - bound), 0.0)
        zsum = jnp.sum(w, axis=1, keepdims=True)
        s = jnp.dot(w.astype(BF16), x, preferred_element_type=F32).astype(BF16)
        for p in range(CORES):
            part[p, b] = s[p * par:(p + 1) * par].reshape(chips, own, width)
        hit = jnp.where(zlane == b, zsum, zpart[...].reshape(slots, 128))
        zpart[...] = hit.reshape(CORES, par, 128)
        return carry

    def combine_row(b):
        slot = b % 2
        if b >= 2:
            pltpu.make_async_copy(cbuf.at[slot], comb_ref.at[b - 2], c_sem.at[slot]).wait()
        logits = lax.dot_general(xnbuf[b], phi_comb[...], NT, preferred_element_type=F32)
        e = jnp.exp(logits)
        total = jnp.sum(e, axis=-1, keepdims=True)
        cbuf[slot] = (e * (1.0 / total)).astype(BF16)
        pltpu.make_async_copy(cbuf.at[slot], comb_ref.at[b], c_sem.at[slot]).start()

    def span(g):
        return pl.ds(g * GROUP_ROWS, GROUP_ROWS)

    def pair_copy(g):
        return pltpu.make_async_remote_copy(
            src_ref=part.at[other, span(g)], dst_ref=pin.at[span(g)], send_sem=pr_send.at[g], recv_sem=pr_recv.at[g],
            device_id={"seq": partner}, device_id_type=MESH)

    def zpair_copy():
        return pltpu.make_async_remote_copy(
            src_ref=zpart.at[other], dst_ref=zpin, send_sem=pr_send.at[groups], recv_sem=pr_recv.at[groups],
            device_id={"seq": partner}, device_id_type=MESH)

    def z_copy(delta):
        return pltpu.make_async_remote_copy(
            src_ref=zchip.at[chip_at(delta)], dst_ref=zrecv.at[delta], send_sem=z_send.at[delta],
            recv_sem=z_recv.at[delta], device_id={"seq": dev_at(delta)}, device_id_type=MESH)

    def steps_of(way, index):
        return far if (index % 2 == 0) == (way == UP) else far - 1

    def sign(way):
        return 1 if way == UP else -1

    def rs_copy(way, g, k):
        if k == steps_of(way, g):
            src = chip.at[span(g), chip_at(sign(way) * k)]
        else:
            src = sbuf.at[way, k, span(g)]
        return pltpu.make_async_remote_copy(
            src_ref=src, dst_ref=rbuf.at[way, k, span(g)], send_sem=rs_send.at[way, g, k], recv_sem=rs_recv.at[way, g, k],
            device_id={"seq": target[way]}, device_id_type=MESH)

    def rs_hop(g, step):
        for way in (UP, DOWN):
            k = steps_of(way, g) - step
            if k < 1:
                continue
            if step:
                rs_copy(way, g, k + 1).wait_recv()
                dest = chip_at(sign(way) * k)
                total = chip[span(g), dest].astype(F32) + rbuf[way, k + 1, span(g)].astype(F32)
                sbuf[way, k, span(g)] = total.astype(BF16)
            rs_copy(way, g, k).start()

    def chip_sum(g):
        pair_copy(g).wait_recv()
        chip[span(g)] = (part[core, span(g)].astype(F32) + pin[span(g)].astype(F32)).astype(BF16)

    for g in range(groups):
        for b in range(g * GROUP_ROWS, (g + 1) * GROUP_ROWS):
            x_copies[b].wait()
        lax.fori_loop(g * GROUP_ROWS, (g + 1) * GROUP_ROWS, dispatch_row, 0)
        if g == 0:
            pl.semaphore_wait(barrier, chips)
        pair_copy(g).start()
        if g == groups - 1:
            zpair_copy().start()
        for step in range(far - 1, 0, -1):
            if 0 <= g - 1 - step:
                rs_hop(g - 1 - step, step)
        if g >= 1:
            chip_sum(g - 1)
            rs_hop(g - 1, 0)

    done = 0
    for r in range(groups, groups + far):
        if r > groups:
            for _ in range(2):
                if done < rows - 1:
                    combine_row(done)
                    done += 1
        for step in range(far - 1, 0, -1):
            g = r - 1 - step
            if 0 <= g < groups:
                rs_hop(g, step)
        if r == groups:
            combine_row(done)
            done += 1
            chip_sum(groups - 1)
            rs_hop(groups - 1, 0)
            zpair_copy().wait_recv()
            zs = zpart[core] + zpin[...]
            zl = lax.broadcasted_iota(jnp.int32, zs.shape, 1)
            hi = zs.astype(BF16).astype(F32)
            mid = (zs - hi).astype(BF16).astype(F32)
            low = zs - hi - mid
            split = jnp.where(zl < rows, hi, 0.0)
            split = split + jnp.where((zl >= rows) & (zl < 2 * rows), pltpu.roll(mid, rows, 1), 0.0)
            split = split + jnp.where((zl >= 2 * rows) & (zl < 3 * rows), pltpu.roll(low, 2 * rows, 1), 0.0)
            zchip[...] = split.astype(BF16).reshape(zchip.shape)
            for delta in range(1, chips):
                z_copy(delta).start()
    while done < rows:
        combine_row(done)
        done += 1

    zsum = zchip[z].astype(F32)
    for delta in range(1, chips):
        z_copy(delta).wait_recv()
        zsum = zsum + zrecv[delta].astype(F32)
    lane = lax.broadcasted_iota(jnp.int32, zsum.shape, 1)
    for g in range(groups):
        rs_copy(UP, g, 1).wait_recv()
        rs_copy(DOWN, g, 1).wait_recv()
        for b in range(g * GROUP_ROWS, (g + 1) * GROUP_ROWS):
            s = chip[b, z].astype(F32) + rbuf[UP, 1, b].astype(F32) + rbuf[DOWN, 1, b].astype(F32)
            mine = (lane % rows == b) & (lane < 3 * rows)
            zb = jnp.sum(jnp.where(mine, zsum, 0.0), axis=-1, keepdims=True)
            slot_in[b * own:(b + 1) * own] = (s / zb).astype(BF16)

    count = rows * own
    i0 = lax.broadcasted_iota(jnp.int32, (count, count), 0)
    i1 = lax.broadcasted_iota(jnp.int32, (count, count), 1)
    rb = rows * per
    src = ((i0 % rb) // per) * own + (i0 // rb) * per + i0 % per
    perm = jnp.where(i1 == src, 1.0, 0.0).astype(BF16)
    by_expert = jnp.dot(perm, slot_in[...], preferred_element_type=F32).astype(BF16)
    hc = half_e * rb
    j0 = lax.broadcasted_iota(jnp.int32, (hc, hc), 0)
    j1 = lax.broadcasted_iota(jnp.int32, (hc, hc), 1)
    back = ((j0 % hs) // per) * rb + (j0 // hs) * per + j0 % per
    unperm = jnp.where(j1 == back, 1.0, 0.0).astype(BF16)

    def ag_copy(way, h, k):
        block = dev_at(-sign(way) * (k - 1))
        return pltpu.make_async_remote_copy(
            src_ref=gath.at[h, :, block], dst_ref=gath.at[h, :, block], send_sem=ag_send.at[way, h, k],
            recv_sem=ag_recv.at[way, h, k], device_id={"seq": target[way]}, device_id_type=MESH)

    def block_copies(h, delta):
        index = delta + far
        block = dev_at(delta)
        remote = pltpu.make_async_remote_copy(
            src_ref=gath.at[h, :, block], dst_ref=gat_ref.at[h, :, block], send_sem=pg_send.at[h, index],
            recv_sem=pg_recv.at[h, index], device_id={"seq": partner}, device_id_type=MESH)
        local = pltpu.make_async_copy(gath.at[h, :, block], gat_ref.at[h, :, block], lg_sem.at[h, index])
        return remote, local

    def publish(h, delta):
        for copy in block_copies(h, delta):
            copy.start()

    def ag_hop(h, k):
        for way in (UP, DOWN):
            if k > 1 and k - 1 <= steps_of(way, h):
                ag_copy(way, h, k - 1).wait_recv()
            if k <= steps_of(way, h):
                ag_copy(way, h, k).start()
        if k == 1:
            publish(h, 0)
        else:
            for way in (UP, DOWN):
                if k - 1 <= steps_of(way, h):
                    publish(h, -sign(way) * (k - 1))

    for h in range(HALVES):
        for copy in w_copies[h]:
            copy.wait()
        for i in range(half_e):
            e = h * half_e + i
            hid = jnp.dot(by_expert[e * rb:(e + 1) * rb], win[e], preferred_element_type=F32)
            hid = jax.nn.gelu(hid).astype(BF16)
            ypart[i * rb:(i + 1) * rb] = jnp.dot(hid, wout[e], preferred_element_type=F32).astype(BF16)
            if h and i == half_e // 2:
                ag_hop(0, 2)
        blk = jnp.dot(unperm, ypart[...], preferred_element_type=F32)
        gath[h, :, me] = blk.reshape(rows, hs, width).astype(BF16)
        ag_hop(h, 1)
    ag_hop(0, 3)
    ag_hop(1, 2)
    ag_hop(0, 4)
    ag_hop(1, 3)
    ag_hop(0, 5)
    ag_hop(1, 4)
    ag_hop(1, 5)

    for h in range(HALVES):
        for delta in range(1 - far, far + 1):
            real = delta
            if delta == far:
                real = -far if steps_of(UP, h) == far else far
            remote, local = block_copies(h, real)
            remote.wait()
            local.wait()
        for way in (UP, DOWN):
            for k in range(1, steps_of(way, h) + 1):
                ag_copy(way, h, k).wait_send()
    for g in range(groups):
        pair_copy(g).wait_send()
        for way in (UP, DOWN):
            for k in range(1, steps_of(way, g) + 1):
                rs_copy(way, g, k).wait_send()
    zpair_copy().wait_send()
    for delta in range(1, chips):
        z_copy(delta).wait_send()
    for b in range(rows - 2, rows):
        pltpu.make_async_copy(cbuf.at[b % 2], comb_ref.at[b], c_sem.at[b % 2]).wait()


def _combine_kernel(len_ref, comb_ref, gat_ref, out_ref):
    b = pl.program_id(0)
    toks = out_ref.shape[1]
    half = gat_ref.shape[2]
    pos = lax.axis_index("seq") * toks + lax.broadcasted_iota(jnp.int32, (toks, 1), 0)
    acc = jnp.dot(comb_ref[0, :, :half], gat_ref[0, 0], preferred_element_type=F32)
    for h in range(1, HALVES):
        acc = acc + jnp.dot(comb_ref[0, :, h * half:(h + 1) * half], gat_ref[h, 0], preferred_element_type=F32)
    out_ref[0] = jnp.where(pos < len_ref[b], acc, 0.0).astype(BF16)


def solution(mesh):
    seq = mesh.shape["seq"]

    def shard_body(tok, lens, params, scale, w_in, w_out):
        rows, toks, width = tok.shape
        slots = params.shape[1]
        experts, _, ff = w_in.shape
        own = slots // seq
        chips = seq // CORES
        groups = rows // GROUP_ROWS
        far = chips // 2
        hs = own // HALVES
        par = slots // CORES
        count = rows * own
        dims = (rows, toks, width, slots, seq, experts, ff)
        dma = pltpu.SemaphoreType.DMA
        any_spec = pl.BlockSpec(memory_space=pl.ANY)
        smem = pl.BlockSpec(memory_space=pltpu.SMEM)
        vmem = pl.BlockSpec(memory_space=pltpu.VMEM)
        comb, gat = pl.pallas_call(
            functools.partial(_exchange_kernel, dims),
            out_shape=(jax.ShapeDtypeStruct((rows, toks, slots), BF16),
                       jax.ShapeDtypeStruct((HALVES, rows, seq, hs, width), BF16)),
            in_specs=[smem, smem, vmem, any_spec, any_spec, any_spec],
            out_specs=(any_spec, any_spec),
            scratch_shapes=[
                pltpu.VMEM((rows, toks, width), BF16),
                pltpu.VMEM((rows, toks, width), BF16),
                pltpu.VMEM((slots, width), BF16),
                pltpu.VMEM((slots, width), BF16),
                pltpu.VMEM((CORES, rows, chips, own, width), BF16),
                pltpu.VMEM((rows, chips, own, width), BF16),
                pltpu.VMEM((rows, chips, own, width), BF16),
                pltpu.VMEM((2, far + 1, rows, own, width), BF16),
                pltpu.VMEM((2, far + 1, rows, own, width), BF16),
                pltpu.VMEM((CORES, par, 128), F32),
                pltpu.VMEM((par, 128), F32),
                pltpu.VMEM((chips, own, 128), BF16),
                pltpu.VMEM((chips, own, 128), BF16),
                pltpu.VMEM((count, width), BF16),
                pltpu.VMEM((experts, width, ff), BF16),
                pltpu.VMEM((experts, ff, width), BF16),
                pltpu.VMEM((HALVES, rows, seq, hs, width), BF16),
                pltpu.VMEM((count // HALVES, width), BF16),
                pltpu.VMEM((2, toks, slots), BF16),
                dma((rows,)), dma((HALVES,)), dma((HALVES,)),
                dma((groups + 1,)), dma((groups + 1,)),
                dma((2, groups, far + 1)), dma((2, groups, far + 1)),
                dma((chips,)), dma((chips,)),
                dma((2, HALVES, far + 1)), dma((2, HALVES, far + 1)),
                dma((HALVES, chips + 1)), dma((HALVES, chips + 1)), dma((HALVES, chips + 1)),
                dma((2,)),
            ],
            compiler_params=pltpu.CompilerParams(
                collective_id=0, has_side_effects=True, vmem_limit_bytes=60 * 1024 * 1024),
            name="exchange",
        )(lens, scale, params, tok, w_in, w_out)
        gat = gat.reshape(HALVES, rows, seq * hs, width)
        return pl.pallas_call(
            _combine_kernel,
            grid=(rows,),
            out_shape=jax.ShapeDtypeStruct((rows, toks, width), BF16),
            in_specs=[smem,
                      pl.BlockSpec((1, toks, slots), lambda b: (b, 0, 0)),
                      pl.BlockSpec((HALVES, 1, seq * hs, width), lambda b: (0, b, 0, 0))],
            out_specs=pl.BlockSpec((1, toks, width), lambda b: (b, 0, 0)),
            compiler_params=pltpu.CompilerParams(dimension_semantics=("arbitrary",)),
            name="combine",
        )(lens, comb, gat)

    return jax.shard_map(
        shard_body,
        mesh=mesh,
        in_specs=(P("data", "seq", None), P("data"), P(None, None), P(None), P("seq", None, None), P("seq", None, None)),
        out_specs=P("data", "seq", None),
        check_vma=False,
    )
```

```python
import functools

import jax
import jax.numpy as jnp
from jax import lax
from jax.experimental import pallas as pl
from jax.experimental.pallas import tpu as pltpu
from jax.sharding import PartitionSpec as P

F32 = jnp.float32
BF16 = jnp.bfloat16
MESH = pl.DeviceIdType.MESH
NT = (((1,), (1,)), ((), ()))
UP, DOWN = 0, 1
GROUP_ROWS = 2
HALVES = 2
CORES = 2
VMEM_LIMIT = 52 * 1024 * 1024
COMBINE_LIMIT = 20 * 1024 * 1024


def _exchange_kernel(dims, len_ref, scale_ref, phi_ref, tok_ref, win_ref, wout_ref, comb_ref, gat_ref,
                     xbuf, xnbuf, phi_ring, phi_comb, part, pin, chip, cbuf, rbuf, zpart, zpin, zchip, zrecv,
                     slot_in, win, wout, ypart,
                     x_sem, w_sem, pr_send, pr_recv, zp_sem, z_sem, relay_recv, fin_recv, rs_send,
                     ag_recv, ag_send, pg_recv):
    rows, toks, width, slots, seq, experts = dims
    chips = seq // CORES
    own = slots // seq
    per = own // experts
    groups = rows // GROUP_ROWS
    far = chips // 2
    half_e = experts // HALVES
    hs = own // HALVES
    par = slots // CORES

    me = lax.axis_index("seq")
    z = me // CORES
    core = me % CORES
    other = 1 - core
    partner = z * CORES + other

    def chip_at(delta):
        return (z + delta + chips) % chips

    def dev_at(delta):
        return chip_at(delta) * CORES + core

    def sign(way):
        return 1 if way == UP else -1

    def remote(src, dst, send, recv, dev):
        return pltpu.make_async_remote_copy(
            src_ref=src, dst_ref=dst, send_sem=send, recv_sem=recv, device_id={"seq": dev}, device_id_type=MESH)

    def wait_bytes(ref, sem):
        pltpu.make_async_copy(ref, ref, sem).wait()

    x_parts = [pl.ds(0, 1), pl.ds(1, 1), pl.ds(2, rows - 2)]
    x_copies = [pltpu.make_async_copy(tok_ref.at[p], xbuf.at[p], x_sem.at[i]) for i, p in enumerate(x_parts)]
    for copy in x_copies:
        copy.start()

    barrier = pltpu.get_barrier_semaphore()
    for delta in range(1, chips):
        pl.semaphore_signal(barrier, inc=1, device_id={"seq": dev_at(delta)}, device_id_type=MESH)
    pl.semaphore_signal(barrier, inc=1, device_id={"seq": partner}, device_id_type=MESH)

    gain = scale_ref[0]
    params = phi_ref[...].astype(F32)
    col_inv = lax.rsqrt(jnp.sum(params * params, axis=0, keepdims=True) + 1e-6)
    phi_norm = (params * (gain * col_inv)).astype(BF16).astype(F32)
    phi_t = phi_norm.T
    ring_order = [phi_t[(d * CORES + p) * own:(d * CORES + p + 1) * own] for p in range(CORES) for d in range(chips)]
    phi_ring[...] = jnp.concatenate(ring_order, axis=0).astype(BF16)
    comb_order = [phi_t[i * own + h * hs:i * own + (h + 1) * hs] for h in range(HALVES) for i in range(seq)]
    phi_comb[...] = jnp.concatenate(comb_order, axis=0).astype(BF16)
    bound = gain * 1.01
    zlane = lax.broadcasted_iota(jnp.int32, (slots, 128), 1)
    zpart[...] = jnp.zeros_like(zpart)

    def dispatch_row(b):
        x = xbuf[b]
        xf = x.astype(F32)
        inv = lax.rsqrt(jnp.sum(xf * xf, axis=-1, keepdims=True) + 1e-6)
        xn = (xf * inv).astype(BF16)
        xnbuf[b] = xn
        lt = lax.dot_general(phi_ring[...], xn, NT, preferred_element_type=F32)
        pos = me * toks + lax.broadcasted_iota(jnp.int32, (1, toks), 1)
        w = jnp.where(pos < len_ref[b], jnp.exp(lt - bound), 0.0)
        zsum = jnp.sum(w, axis=1, keepdims=True)
        s = jnp.dot(w.astype(BF16), x, preferred_element_type=F32).astype(BF16)
        for p in range(CORES):
            part[p, b] = s[p * par:(p + 1) * par].reshape(chips, own, width)
        hit = jnp.where(zlane == b, zsum, zpart[...].reshape(slots, 128))
        zpart[...] = hit.reshape(CORES, par, 128)

    def combine_row(b):
        logits = lax.dot_general(xnbuf[b], phi_comb[...], NT, preferred_element_type=F32)
        e = jnp.exp(logits)
        total = jnp.sum(e, axis=-1, keepdims=True)
        comb_ref[b] = (e * (1.0 / total)).astype(BF16)

    def span(g):
        return pl.ds(g * GROUP_ROWS, GROUP_ROWS)

    def pair_copy(g):
        return remote(part.at[other, span(g)], pin.at[span(g)], pr_send, pr_recv.at[g], partner)

    def zpair_copy():
        return remote(zpart.at[other], zpin, zp_sem.at[0], zp_sem.at[1], partner)

    def chip_sum(g):
        pair_copy(g).wait_recv()
        chip[span(g)] = (part[core, span(g)].astype(F32) + pin[span(g)].astype(F32)).astype(BF16)

    def is_far(way, index):
        return (index % 2 == 0) == (way == UP)

    def rs_first(g):
        for way in (UP, DOWN):
            s = sign(way)
            relay = relay_recv.at[way, g]
            if is_far(way, g):
                remote(chip.at[span(g), chip_at(far * s)], rbuf.at[way, 0, span(g)], rs_send, relay, dev_at(2 * s)).start()
            remote(chip.at[span(g), chip_at(3 * s)], rbuf.at[way, 1, span(g)], rs_send, relay, dev_at(s)).start()
        for way in (UP, DOWN):
            s = sign(way)
            remote(chip.at[span(g), chip_at(s)], rbuf.at[way, 3, span(g)], rs_send, fin_recv, dev_at(s)).start()

    def rs_relay(g):
        for way in (UP, DOWN):
            s = sign(way)
            first = 0 if is_far(way, g) else 1
            wait_bytes(rbuf.at[way, pl.ds(first, 2 - first), span(g)], relay_recv.at[way, g])
            total = chip[span(g), chip_at(2 * s)].astype(F32)
            for kind in range(first, 2):
                total = total + rbuf[way, kind, span(g)].astype(F32)
            cbuf[way, span(g)] = total.astype(BF16)
            remote(cbuf.at[way, span(g)], rbuf.at[way, 2, span(g)], rs_send, fin_recv, dev_at(2 * s)).start()

    def z_exchange():
        zpair_copy().wait_recv()
        zs = zpart[core] + zpin[...]
        zl = lax.broadcasted_iota(jnp.int32, zs.shape, 1)
        hi = zs.astype(BF16).astype(F32)
        mid = (zs - hi).astype(BF16).astype(F32)
        low = zs - hi - mid
        split = jnp.where(zl < rows, hi, 0.0)
        split = split + jnp.where((zl >= rows) & (zl < 2 * rows), pltpu.roll(mid, rows, 1), 0.0)
        split = split + jnp.where((zl >= 2 * rows) & (zl < 3 * rows), pltpu.roll(low, 2 * rows, 1), 0.0)
        zchip[...] = split.astype(BF16).reshape(zchip.shape)
        for delta in range(1, chips):
            remote(zchip.at[chip_at(delta)], zrecv.at[delta], z_sem.at[0], z_sem.at[1], dev_at(delta)).start()

    def weights(h):
        es = pl.ds(h * half_e, half_e)
        return (pltpu.make_async_copy(win_ref.at[es], win.at[es], w_sem.at[h]),
                pltpu.make_async_copy(wout_ref.at[es], wout.at[es], w_sem.at[h]))

    for b in range(rows):
        if b < len(x_parts):
            with jax.named_scope(f"x{b}"):
                x_copies[b].wait()
        with jax.named_scope(f"disp{b}"):
            dispatch_row(b)
        if b == 1:
            for h in range(HALVES):
                for copy in weights(h):
                    copy.start()
            with jax.named_scope("barrier"):
                pl.semaphore_wait(barrier, chips)
        g = b // GROUP_ROWS
        if b % GROUP_ROWS == GROUP_ROWS - 1:
            pair_copy(g).start()
            if b == rows - 1:
                zpair_copy().start()
        elif g >= 1:
            with jax.named_scope(f"sum{g - 1}"):
                chip_sum(g - 1)
                rs_first(g - 1)
        if b == rows - 2:
            with jax.named_scope("relay0"):
                rs_relay(0)

    def comb(b):
        with jax.named_scope(f"comb{b}"):
            combine_row(b)

    def relay(g):
        with jax.named_scope(f"relay{g}"):
            rs_relay(g)

    comb(0)
    with jax.named_scope(f"sum{groups - 1}"):
        chip_sum(groups - 1)
        rs_first(groups - 1)
    relay(1)
    z_exchange()
    comb(1)
    comb(2)
    relay(2)
    comb(3)
    comb(4)
    relay(3)
    comb(5)
    comb(6)
    comb(7)

    with jax.named_scope("zwait"):
        wait_bytes(zrecv.at[pl.ds(1, chips - 1)], z_sem.at[1])
    with jax.named_scope("finwait"):
        wait_bytes(rbuf.at[:, pl.ds(2, 2)], fin_recv)
    zsum = zchip[z].astype(F32)
    for delta in range(1, chips):
        zsum = zsum + zrecv[delta].astype(F32)
    lane = lax.broadcasted_iota(jnp.int32, zsum.shape, 1)
    for b in range(rows):
        s = chip[b, z].astype(F32)
        for way in (UP, DOWN):
            s = s + (rbuf[way, 2, b].astype(F32) + rbuf[way, 3, b].astype(F32))
        mine = (lane % rows == b) & (lane < 3 * rows)
        zb = jnp.sum(jnp.where(mine, zsum, 0.0), axis=-1, keepdims=True)
        slot_in[b * own:(b + 1) * own] = (s / zb).astype(BF16)

    count = rows * own
    i0 = lax.broadcasted_iota(jnp.int32, (count, count), 0)
    i1 = lax.broadcasted_iota(jnp.int32, (count, count), 1)
    rb = rows * per
    src = ((i0 % rb) // per) * own + (i0 // rb) * per + i0 % per
    perm = jnp.where(i1 == src, 1.0, 0.0).astype(BF16)
    by_expert = jnp.dot(perm, slot_in[...], preferred_element_type=F32).astype(BF16)
    hc = half_e * rb
    j0 = lax.broadcasted_iota(jnp.int32, (hc, hc), 0)
    j1 = lax.broadcasted_iota(jnp.int32, (hc, hc), 1)
    back = ((j0 % hs) // per) * rb + (j0 // hs) * per + j0 % per
    unperm = jnp.where(j1 == back, 1.0, 0.0).astype(BF16)

    def block(h, delta):
        return gat_ref.at[:, h, dev_at(delta)]

    def send(h, delta, way, kind, to):
        remote(block(h, delta), block(h, delta), ag_send, ag_recv.at[h, way, kind], dev_at(to)).start()

    def arrived(h, way, kind):
        with jax.named_scope(f"ag_h{h}_w{way}_k{kind}"):
            wait_bytes(block(h, 0), ag_recv.at[h, way, kind])

    def publish(h, delta):
        remote(block(h, delta), block(h, delta), ag_send, pg_recv, partner).start()

    def ring(h, k):
        for way in (UP, DOWN):
            s = sign(way)
            last = far if is_far(way, h) else far - 1
            if k > 1 and k - 1 <= last:
                arrived(h, way, k - 2)
            if k <= last:
                send(h, -s * (k - 1), way, k - 1, s)
            if k > 1 and k - 1 <= last:
                publish(h, -s * (k - 1))
        if k == 1:
            publish(h, 0)

    def direct(h):
        for way in (UP, DOWN):
            send(h, 0, way, 1, 2 * sign(way))
        for way in (UP, DOWN):
            send(h, 0, way, 0, sign(way))
        publish(h, 0)

    def forward(h):
        for way in (UP, DOWN):
            s = sign(way)
            arrived(h, way, 1)
            if is_far(way, h):
                send(h, -2 * s, way, 3, 2 * s)
            send(h, -2 * s, way, 2, s)
            publish(h, -2 * s)
        for way in (UP, DOWN):
            arrived(h, way, 0)
            publish(h, -sign(way))

    def collect(h):
        for way in (UP, DOWN):
            arrived(h, way, 2)
            publish(h, -3 * sign(way))
        for way in (UP, DOWN):
            if is_far(way, h):
                arrived(h, way, 3)
                publish(h, -far * sign(way))

    for h in range(HALVES):
        with jax.named_scope(f"wwait{h}"):
            wait_bytes(win, w_sem.at[h])
        with jax.named_scope(f"ffn{h}"):
            for i in range(half_e):
                e = h * half_e + i
                hid = jnp.dot(by_expert[e * rb:(e + 1) * rb], win[e], preferred_element_type=F32)
                hid = jax.nn.gelu(hid).astype(BF16)
                ypart[i * rb:(i + 1) * rb] = jnp.dot(hid, wout[e], preferred_element_type=F32).astype(BF16)
            blk = jnp.dot(unperm, ypart[...], preferred_element_type=F32)
            gat_ref[:, h, me] = blk.reshape(rows, hs, width).astype(BF16)
        if h == 0:
            ring(0, 1)
        else:
            direct(1)
    ring(0, 2)
    ring(0, 3)
    forward(1)
    ring(0, 4)
    ring(0, 5)
    collect(1)

    with jax.named_scope("end"):
        wait_bytes(gat_ref.at[:, :, pl.ds(0, chips)], pg_recv)
        wait_bytes(gat_ref.at[:, :, pl.ds(0, seq - 1)], ag_send)
        wait_bytes(pin, pr_send)
        zpair_copy().wait_send()
        wait_bytes(zrecv.at[pl.ds(1, chips - 1)], z_sem.at[0])
        wait_bytes(part.at[0, :, pl.ds(0, chips - 1)], rs_send)


def _combine_kernel(len_ref, comb_ref, gat_ref, out_ref, ybuf, y_sem):
    rows, toks, width = ybuf.shape
    pos = lax.axis_index("seq") * toks + lax.broadcasted_iota(jnp.int32, (toks, 1), 0)

    def out_copy(b):
        return pltpu.make_async_copy(ybuf.at[b], out_ref.at[b], y_sem.at[b])

    for b in range(rows):
        acc = jnp.dot(comb_ref[b], gat_ref[b], preferred_element_type=F32)
        ybuf[b] = jnp.where(pos < len_ref[b], acc, 0.0).astype(BF16)
        out_copy(b).start()
    for b in range(rows):
        out_copy(b).wait()


def solution(mesh):
    seq = mesh.shape["seq"]

    def shard_body(tok, lens, params, scale, w_in, w_out):
        rows, toks, width = tok.shape
        slots = params.shape[1]
        experts, _, ff = w_in.shape
        own = slots // seq
        chips = seq // CORES
        groups = rows // GROUP_ROWS
        hs = own // HALVES
        par = slots // CORES
        count = rows * own
        dims = (rows, toks, width, slots, seq, experts)
        dma = pltpu.SemaphoreType.DMA
        any_spec = pl.BlockSpec(memory_space=pl.ANY)
        smem = pl.BlockSpec(memory_space=pltpu.SMEM)
        vmem = pl.BlockSpec(memory_space=pltpu.VMEM)
        comb, gat = pl.pallas_call(
            functools.partial(_exchange_kernel, dims),
            out_shape=(pltpu.VMEM((rows, toks, slots), BF16),
                       pltpu.VMEM((rows, HALVES, seq, hs, width), BF16)),
            in_specs=[smem, smem, vmem, any_spec, any_spec, any_spec],
            out_specs=(vmem, vmem),
            scratch_shapes=[
                pltpu.VMEM((rows, toks, width), BF16),
                pltpu.VMEM((rows, toks, width), BF16),
                pltpu.VMEM((slots, width), BF16),
                pltpu.VMEM((slots, width), BF16),
                pltpu.VMEM((CORES, rows, chips, own, width), BF16),
                pltpu.VMEM((rows, chips, own, width), BF16),
                pltpu.VMEM((rows, chips, own, width), BF16),
                pltpu.VMEM((2, rows, own, width), BF16),
                pltpu.VMEM((2, 4, rows, own, width), BF16),
                pltpu.VMEM((CORES, par, 128), F32),
                pltpu.VMEM((par, 128), F32),
                pltpu.VMEM((chips, own, 128), BF16),
                pltpu.VMEM((chips, own, 128), BF16),
                pltpu.VMEM((count, width), BF16),
                pltpu.VMEM((experts, width, ff), BF16),
                pltpu.VMEM((experts, ff, width), BF16),
                pltpu.VMEM((count // HALVES, width), BF16),
                dma((3,)), dma((HALVES,)), dma, dma((groups,)), dma((2,)), dma((2,)),
                dma((2, groups)), dma, dma, dma((HALVES, 2, 4)), dma, dma,
            ],
            compiler_params=pltpu.CompilerParams(
                collective_id=0, has_side_effects=True, vmem_limit_bytes=VMEM_LIMIT),
            name="exchange",
        )(lens, scale, params, tok, w_in, w_out)
        gat = gat.reshape(rows, slots, width)
        return pl.pallas_call(
            _combine_kernel,
            out_shape=jax.ShapeDtypeStruct((rows, toks, width), BF16),
            in_specs=[smem, vmem, vmem],
            out_specs=any_spec,
            scratch_shapes=[pltpu.VMEM((rows, toks, width), BF16), dma((rows,))],
            compiler_params=pltpu.CompilerParams(vmem_limit_bytes=COMBINE_LIMIT),
            name="combine",
        )(lens, comb, gat)

    return jax.shard_map(
        shard_body,
        mesh=mesh,
        in_specs=(P("data", "seq", None), P("data"), P(None, None), P(None), P("seq", None, None), P("seq", None, None)),
        out_specs=P("data", "seq", None),
        check_vma=False,
    )
```

```python
import functools

import jax
import jax.numpy as jnp
from jax import lax
from jax.experimental import pallas as pl
from jax.experimental.pallas import tpu as pltpu
from jax.sharding import PartitionSpec as P

F32 = jnp.float32
BF16 = jnp.bfloat16
MESH = pl.DeviceIdType.MESH
NT = (((1,), (1,)), ((), ()))
UP, DOWN = 0, 1
GROUP_ROWS = 2
HALVES = 2
CORES = 2
RING_GROUPS = 2
CHUNKS = 2
VMEM_LIMIT = 52 * 1024 * 1024
COMBINE_LIMIT = 20 * 1024 * 1024


def _exchange_kernel(dims, len_ref, scale_ref, phi_ref, tok_ref, win_ref, wout_ref, comb_ref, gat_ref,
                     xbuf, xnbuf, phi_in, phi_ring, phi_comb, part, pin, chip, cbuf, rbuf, hsend, hrecv, zpart, zpin, zchip, zrecv,
                     slot_in, win, wout, ypart,
                     x_sem, phi_sem, w_sem, pr_send, pr_recv, zp_sem, z_sem, relay_recv, hop_recv, fin_recv, hfin_recv, rs_send,
                     ag_recv, ag_send, pg_recv):
    rows, toks, width, slots, seq, experts = dims
    chips = seq // CORES
    own = slots // seq
    per = own // experts
    groups = rows // GROUP_ROWS
    far = chips // 2
    half_e = experts // HALVES
    hs = own // HALVES
    par = slots // CORES

    me = lax.axis_index("seq")
    z = me // CORES
    core = me % CORES
    other = 1 - core
    partner = z * CORES + other

    def chip_at(delta):
        return (z + delta + chips) % chips

    def dev_at(delta):
        return chip_at(delta) * CORES + core

    def sign(way):
        return 1 if way == UP else -1

    def remote(src, dst, send, recv, dev):
        return pltpu.make_async_remote_copy(
            src_ref=src, dst_ref=dst, send_sem=send, recv_sem=recv, device_id={"seq": dev}, device_id_type=MESH)

    def wait_bytes(ref, sem):
        pltpu.make_async_copy(ref, ref, sem).wait()

    x_parts = [pl.ds(0, 1), pl.ds(1, 1), pl.ds(2, rows - 2)]
    x_copies = [pltpu.make_async_copy(tok_ref.at[p], xbuf.at[p], x_sem.at[i]) for i, p in enumerate(x_parts)]
    phi_copy = pltpu.make_async_copy(phi_ref, phi_in, phi_sem)
    phi_copy.start()
    for copy in x_copies:
        copy.start()

    barrier = pltpu.get_barrier_semaphore()
    for delta in range(1, chips):
        pl.semaphore_signal(barrier, inc=1, device_id={"seq": dev_at(delta)}, device_id_type=MESH)
    pl.semaphore_signal(barrier, inc=1, device_id={"seq": partner}, device_id_type=MESH)

    n0 = lax.broadcasted_iota(jnp.int32, (slots, slots), 0)
    n1 = lax.broadcasted_iota(jnp.int32, (slots, slots), 1)
    ring_src = ((n0 % par) // own * CORES + n0 // par) * own + n0 % own
    comb_src = (n0 % (seq * hs)) // hs * own + n0 // (seq * hs) * hs + n0 % hs
    ring_hot = jnp.where(n1 == ring_src, 1.0, 0.0).astype(BF16)
    comb_hot = jnp.where(n1 == comb_src, 1.0, 0.0).astype(BF16)
    gain = scale_ref[0]
    with jax.named_scope("phiwait"):
        phi_copy.wait()
    params = phi_in[...].astype(F32)
    col_inv = lax.rsqrt(jnp.sum(params * params, axis=0, keepdims=True) + 1e-6)
    phi_norm = (params * (gain * col_inv)).astype(BF16)
    phi_ring[...] = lax.dot_general(ring_hot, phi_norm, NT, preferred_element_type=F32).astype(BF16)
    phi_comb[...] = lax.dot_general(comb_hot, phi_norm, NT, preferred_element_type=F32).astype(BF16)
    bound = gain * 1.01
    zlane = lax.broadcasted_iota(jnp.int32, (slots, 128), 1)
    zpart[...] = jnp.zeros_like(zpart)

    def normalize_row(b):
        xf = xbuf[b].astype(F32)
        inv = lax.rsqrt(jnp.sum(xf * xf, axis=-1, keepdims=True) + 1e-6)
        xnbuf[b] = (xf * inv).astype(BF16)

    def dispatch_row(b):
        x = xbuf[b]
        lt = lax.dot_general(phi_ring[...], xnbuf[b], NT, preferred_element_type=F32)
        pos = me * toks + lax.broadcasted_iota(jnp.int32, (1, toks), 1)
        w = jnp.where(pos < len_ref[b], jnp.exp(lt - bound), 0.0)
        zsum = jnp.sum(w, axis=1, keepdims=True)
        s = jnp.dot(w.astype(BF16), x, preferred_element_type=F32).astype(BF16)
        for p in range(CORES):
            part[p, b] = s[p * par:(p + 1) * par].reshape(chips, own, width)
        hit = jnp.where(zlane == b, zsum, zpart[...].reshape(slots, 128))
        zpart[...] = hit.reshape(CORES, par, 128)

    def combine_row(b):
        logits = lax.dot_general(xnbuf[b], phi_comb[...], NT, preferred_element_type=F32)
        e = jnp.exp(logits)
        total = jnp.sum(e, axis=-1, keepdims=True)
        comb_ref[b] = (e * (1.0 / total)).astype(BF16)

    def span(g):
        return pl.ds(g * GROUP_ROWS, GROUP_ROWS)

    def pair_copy(g):
        return remote(part.at[other, span(g)], pin.at[span(g)], pr_send, pr_recv.at[g], partner)

    def zpair_copy():
        return remote(zpart.at[other], zpin, zp_sem.at[0], zp_sem.at[1], partner)

    def chip_sum(g):
        pair_copy(g).wait_recv()
        chip[span(g)] = (part[core, span(g)].astype(F32) + pin[span(g)].astype(F32)).astype(BF16)

    def is_far(way, index):
        return (index % 2 == 0) == (way == UP)

    def last_of(way, index):
        return far if is_far(way, index) else far - 1

    def hop(g, step):
        for way in (UP, DOWN):
            s = sign(way)
            k = last_of(way, g) - step
            if k < 1:
                continue
            if step == 0:
                src = chip.at[span(g), chip_at(s * k)]
            else:
                with jax.named_scope(f"hop{g}_{step}_{way}"):
                    wait_bytes(hrecv.at[way, k + 1, span(g)], hop_recv.at[way, g, k - 1])
                total = chip[span(g), chip_at(s * k)].astype(F32) + hrecv[way, k + 1, span(g)].astype(F32)
                hsend[way, k, span(g)] = total.astype(BF16)
                src = hsend.at[way, k, span(g)]
            recv = hfin_recv if k == 1 else hop_recv.at[way, g, k - 2]
            remote(src, hrecv.at[way, k, span(g)], rs_send, recv, dev_at(s)).start()

    def late(g):
        return pl.ds((g - RING_GROUPS) * GROUP_ROWS, GROUP_ROWS)

    def rs_first(g):
        for way in (UP, DOWN):
            s = sign(way)
            relay = relay_recv.at[way, g - RING_GROUPS]
            if is_far(way, g):
                remote(chip.at[span(g), chip_at(far * s)], rbuf.at[way, 0, late(g)], rs_send, relay, dev_at(2 * s)).start()
            remote(chip.at[span(g), chip_at(3 * s)], rbuf.at[way, 1, late(g)], rs_send, relay, dev_at(s)).start()
        for way in (UP, DOWN):
            s = sign(way)
            remote(chip.at[span(g), chip_at(s)], rbuf.at[way, 3, late(g)], rs_send, fin_recv, dev_at(s)).start()

    def rs_relay(g):
        for way in (UP, DOWN):
            s = sign(way)
            first = 0 if is_far(way, g) else 1
            with jax.named_scope(f"relay{g}_{way}"):
                wait_bytes(rbuf.at[way, pl.ds(first, 2 - first), late(g)], relay_recv.at[way, g - RING_GROUPS])
            total = chip[span(g), chip_at(2 * s)].astype(F32)
            for kind in range(first, 2):
                total = total + rbuf[way, kind, late(g)].astype(F32)
            cbuf[way, late(g)] = total.astype(BF16)
            remote(cbuf.at[way, late(g)], rbuf.at[way, 2, late(g)], rs_send, fin_recv, dev_at(2 * s)).start()

    def z_exchange():
        zpair_copy().wait_recv()
        zs = zpart[core] + zpin[...]
        zl = lax.broadcasted_iota(jnp.int32, zs.shape, 1)
        hi = zs.astype(BF16).astype(F32)
        mid = (zs - hi).astype(BF16).astype(F32)
        low = zs - hi - mid
        split = jnp.where(zl < rows, hi, 0.0)
        split = split + jnp.where((zl >= rows) & (zl < 2 * rows), pltpu.roll(mid, rows, 1), 0.0)
        split = split + jnp.where((zl >= 2 * rows) & (zl < 3 * rows), pltpu.roll(low, 2 * rows, 1), 0.0)
        zchip[...] = split.astype(BF16).reshape(zchip.shape)
        for delta in range(1, chips):
            remote(zchip.at[chip_at(delta)], zrecv.at[delta], z_sem.at[0], z_sem.at[1], dev_at(delta)).start()

    def weights(h):
        es = pl.ds(h * half_e, half_e)
        return (pltpu.make_async_copy(win_ref.at[es], win.at[es], w_sem.at[h]),
                pltpu.make_async_copy(wout_ref.at[es], wout.at[es], w_sem.at[h]))

    def disp(b):
        if b + 1 < len(x_parts):
            with jax.named_scope(f"x{b + 1}"):
                x_copies[b + 1].wait()
        with jax.named_scope(f"disp{b}"):
            if b + 1 < rows:
                normalize_row(b + 1)
            dispatch_row(b)

    def comb(b):
        with jax.named_scope(f"comb{b}"):
            combine_row(b)

    def total(g):
        with jax.named_scope(f"sum{g}"):
            chip_sum(g)

    with jax.named_scope("x0"):
        x_copies[0].wait()
    with jax.named_scope("norm0"):
        normalize_row(0)
    disp(0)
    disp(1)
    for h in range(HALVES):
        for copy in weights(h):
            copy.start()
    disp(2)
    with jax.named_scope("barrier"):
        pl.semaphore_wait(barrier, chips)
    pair_copy(0).start()
    disp(3)
    pair_copy(1).start()
    total(0)
    hop(0, 0)
    disp(4)
    total(1)
    hop(1, 0)
    disp(5)
    pair_copy(2).start()
    disp(6)
    hop(0, 1)
    total(2)
    rs_first(2)
    disp(7)
    pair_copy(3).start()
    zpair_copy().start()
    hop(1, 1)
    comb(0)
    total(3)
    z_exchange()
    rs_first(3)
    hop(0, 2)
    comb(1)
    hop(1, 2)
    rs_relay(2)
    comb(2)
    hop(0, 3)
    rs_relay(3)
    hop(1, 3)
    comb(3)

    with jax.named_scope("zwait"):
        wait_bytes(zrecv.at[pl.ds(1, chips - 1)], z_sem.at[1])
    zsum = zchip[z].astype(F32)
    for delta in range(1, chips):
        zsum = zsum + zrecv[delta].astype(F32)
    lane = lax.broadcasted_iota(jnp.int32, zsum.shape, 1)
    with jax.named_scope("hfin"):
        wait_bytes(hrecv.at[:, 1], hfin_recv)
    with jax.named_scope("fin"):
        wait_bytes(rbuf.at[:, pl.ds(2, 2)], fin_recv)
    for b in range(rows):
        s = chip[b, z].astype(F32)
        for way in (UP, DOWN):
            if b < RING_GROUPS * GROUP_ROWS:
                s = s + hrecv[way, 1, b].astype(F32)
            else:
                lb = b - RING_GROUPS * GROUP_ROWS
                s = s + (rbuf[way, 2, lb].astype(F32) + rbuf[way, 3, lb].astype(F32))
        mine = (lane % rows == b) & (lane < 3 * rows)
        zb = jnp.sum(jnp.where(mine, zsum, 0.0), axis=-1, keepdims=True)
        slot_in[b * own:(b + 1) * own] = (s / zb).astype(BF16)

    count = rows * own
    i0 = lax.broadcasted_iota(jnp.int32, (count, count), 0)
    i1 = lax.broadcasted_iota(jnp.int32, (count, count), 1)
    rb = rows * per
    src = ((i0 % rb) // per) * own + (i0 // rb) * per + i0 % per
    perm = jnp.where(i1 == src, 1.0, 0.0).astype(BF16)
    by_expert = jnp.dot(perm, slot_in[...], preferred_element_type=F32).astype(BF16)
    hc = half_e * rb
    j0 = lax.broadcasted_iota(jnp.int32, (hc, hc), 0)
    j1 = lax.broadcasted_iota(jnp.int32, (hc, hc), 1)
    back = ((j0 % hs) // per) * rb + (j0 // hs) * per + j0 % per
    unperm = jnp.where(j1 == back, 1.0, 0.0).astype(BF16)

    crows = rows // CHUNKS

    def block(h, c, delta):
        return gat_ref.at[pl.ds(c * crows, crows), h, dev_at(delta)]

    def send(h, c, delta, way, kind, to):
        remote(block(h, c, delta), block(h, c, delta), ag_send, ag_recv.at[h, c, way, kind], dev_at(to)).start()

    def arrived(h, c, way, kind):
        with jax.named_scope(f"ag_h{h}_c{c}_w{way}_k{kind}"):
            wait_bytes(block(h, c, 0), ag_recv.at[h, c, way, kind])

    def publish(h, c, delta):
        remote(block(h, c, delta), block(h, c, delta), ag_send, pg_recv, partner).start()

    def ring(c, k):
        for way in (UP, DOWN):
            s = sign(way)
            last = last_of(way, c)
            if k > 1 and k - 1 <= last:
                arrived(0, c, way, k - 2)
            if k <= last:
                send(0, c, -s * (k - 1), way, k - 1, s)
            if k > 1 and k - 1 <= last:
                publish(0, c, -s * (k - 1))
        if k == 1:
            publish(0, c, 0)

    def direct_far(c):
        for way in (UP, DOWN):
            send(1, c, 0, way, 1, 2 * sign(way))

    def direct_near(c):
        for way in (UP, DOWN):
            send(1, c, 0, way, 0, sign(way))
        publish(1, c, 0)

    def forward(c):
        for way in (UP, DOWN):
            s = sign(way)
            arrived(1, c, way, 1)
            if is_far(way, c):
                send(1, c, -2 * s, way, 3, 2 * s)
            send(1, c, -2 * s, way, 2, s)
            publish(1, c, -2 * s)

    def near(c):
        for way in (UP, DOWN):
            arrived(1, c, way, 0)
            publish(1, c, -sign(way))

    def collect(c):
        for way in (UP, DOWN):
            arrived(1, c, way, 2)
            publish(1, c, -3 * sign(way))
        for way in (UP, DOWN):
            if is_far(way, c):
                arrived(1, c, way, 3)
                publish(1, c, -far * sign(way))

    def expert_half(h):
        with jax.named_scope(f"wwait{h}"):
            wait_bytes(win, w_sem.at[h])
        with jax.named_scope(f"ffn{h}"):
            for i in range(half_e):
                e = h * half_e + i
                hid = jnp.dot(by_expert[e * rb:(e + 1) * rb], win[e], preferred_element_type=F32)
                hid = jax.nn.gelu(hid).astype(BF16)
                ypart[i * rb:(i + 1) * rb] = jnp.dot(hid, wout[e], preferred_element_type=F32).astype(BF16)
            blk = jnp.dot(unperm, ypart[...], preferred_element_type=F32)
            gat_ref[:, h, me] = blk.reshape(rows, hs, width).astype(BF16)

    expert_half(0)
    ring(0, 1)
    ring(1, 1)
    expert_half(1)
    direct_far(0)
    direct_far(1)
    comb(4)
    ring(0, 2)
    ring(1, 2)
    direct_near(0)
    direct_near(1)
    comb(5)
    forward(0)
    forward(1)
    ring(0, 3)
    ring(1, 3)
    comb(6)
    near(0)
    near(1)
    comb(7)
    ring(0, 4)
    ring(1, 4)
    collect(0)
    collect(1)
    ring(0, 5)
    ring(1, 5)

    with jax.named_scope("end"):
        wait_bytes(gat_ref.at[:, :, pl.ds(0, chips)], pg_recv)
        wait_bytes(gat_ref.at[:, :, pl.ds(0, seq - 1)], ag_send)
        wait_bytes(pin, pr_send)
        zpair_copy().wait_send()
        wait_bytes(zrecv.at[pl.ds(1, chips - 1)], z_sem.at[0])
        wait_bytes(part.at[0, :, pl.ds(0, chips - 1)], rs_send)


def _combine_kernel(len_ref, comb_ref, gat_ref, out_ref, ybuf, y_sem):
    rows, toks, width = ybuf.shape
    pos = lax.axis_index("seq") * toks + lax.broadcasted_iota(jnp.int32, (toks, 1), 0)

    def out_copy(b):
        return pltpu.make_async_copy(ybuf.at[b], out_ref.at[b], y_sem.at[b])

    for b in range(rows):
        acc = jnp.dot(comb_ref[b], gat_ref[b], preferred_element_type=F32)
        ybuf[b] = jnp.where(pos < len_ref[b], acc, 0.0).astype(BF16)
        out_copy(b).start()
    for b in range(rows):
        out_copy(b).wait()


def solution(mesh):
    seq = mesh.shape["seq"]

    def shard_body(tok, lens, params, scale, w_in, w_out):
        rows, toks, width = tok.shape
        slots = params.shape[1]
        experts, _, ff = w_in.shape
        own = slots // seq
        chips = seq // CORES
        groups = rows // GROUP_ROWS
        ring_rows = RING_GROUPS * GROUP_ROWS
        far = chips // 2
        hs = own // HALVES
        par = slots // CORES
        count = rows * own
        dims = (rows, toks, width, slots, seq, experts)
        dma = pltpu.SemaphoreType.DMA
        any_spec = pl.BlockSpec(memory_space=pl.ANY)
        smem = pl.BlockSpec(memory_space=pltpu.SMEM)
        vmem = pl.BlockSpec(memory_space=pltpu.VMEM)
        comb, gat = pl.pallas_call(
            functools.partial(_exchange_kernel, dims),
            out_shape=(pltpu.VMEM((rows, toks, slots), BF16),
                       pltpu.VMEM((rows, HALVES, seq, hs, width), BF16)),
            in_specs=[smem, smem, any_spec, any_spec, any_spec, any_spec],
            out_specs=(vmem, vmem),
            scratch_shapes=[
                pltpu.VMEM((rows, toks, width), BF16),
                pltpu.VMEM((rows, toks, width), BF16),
                pltpu.VMEM((width, slots), BF16),
                pltpu.VMEM((slots, width), BF16),
                pltpu.VMEM((slots, width), BF16),
                pltpu.VMEM((CORES, rows, chips, own, width), BF16),
                pltpu.VMEM((rows, chips, own, width), BF16),
                pltpu.VMEM((rows, chips, own, width), BF16),
                pltpu.VMEM((2, rows - ring_rows, own, width), BF16),
                pltpu.VMEM((2, 4, rows - ring_rows, own, width), BF16),
                pltpu.VMEM((2, far, ring_rows, own, width), BF16),
                pltpu.VMEM((2, far + 1, ring_rows, own, width), BF16),
                pltpu.VMEM((CORES, par, 128), F32),
                pltpu.VMEM((par, 128), F32),
                pltpu.VMEM((chips, own, 128), BF16),
                pltpu.VMEM((chips, own, 128), BF16),
                pltpu.VMEM((count, width), BF16),
                pltpu.VMEM((experts, width, ff), BF16),
                pltpu.VMEM((experts, ff, width), BF16),
                pltpu.VMEM((count // HALVES, width), BF16),
                dma((3,)), dma, dma((HALVES,)), dma, dma((groups,)), dma((2,)), dma((2,)),
                dma((2, groups - RING_GROUPS)), dma((2, RING_GROUPS, far - 1)), dma, dma, dma,
                dma((HALVES, CHUNKS, 2, 4)), dma, dma,
            ],
            compiler_params=pltpu.CompilerParams(
                collective_id=0, has_side_effects=True, vmem_limit_bytes=VMEM_LIMIT),
            name="exchange",
        )(lens, scale, params, tok, w_in, w_out)
        gat = gat.reshape(rows, slots, width)
        return pl.pallas_call(
            _combine_kernel,
            out_shape=jax.ShapeDtypeStruct((rows, toks, width), BF16),
            in_specs=[smem, vmem, vmem],
            out_specs=any_spec,
            scratch_shapes=[pltpu.VMEM((rows, toks, width), BF16), dma((rows,))],
            compiler_params=pltpu.CompilerParams(vmem_limit_bytes=COMBINE_LIMIT),
            name="combine",
        )(lens, comb, gat)

    return jax.shard_map(
        shard_body,
        mesh=mesh,
        in_specs=(P("data", "seq", None), P("data"), P(None, None), P(None), P("seq", None, None), P("seq", None, None)),
        out_specs=P("data", "seq", None),
        check_vma=False,
    )
```

```python
import functools

import jax
import jax.numpy as jnp
from jax import lax
from jax.experimental import pallas as pl
from jax.experimental.pallas import tpu as pltpu
from jax.sharding import PartitionSpec as P

F32 = jnp.float32
BF16 = jnp.bfloat16
MESH = pl.DeviceIdType.MESH
NT = (((1,), (1,)), ((), ()))
UP, DOWN = 0, 1
GROUP_ROWS = 2
HALVES = 2
CORES = 2
CHUNKS = 2
RS_PLAN = "TTTT"
ORDER = (
    ("disp", 0), ("disp", 1), ("bar",), ("disp", 2), ("pair", 0), ("disp", 3), ("disp", 4), ("pair", 1),
    ("total", 0), ("first", 0), ("disp", 5), ("disp", 6), ("pair", 2), ("total", 1), ("first", 1), ("disp", 7),
    ("disp", 8), ("total", 2), ("first", 2), ("pair", 3), ("total", 3), ("zpair",), ("first", 3), ("relay", 0),
    ("z",), ("comb", 0), ("comb", 1), ("comb", 2), ("relay", 2), ("relay", 1), ("comb", 3), ("relay", 3),
    ("comb", 4), ("comb", 5), ("FIN",), ("ffn", 0), ("ring", 0, 0, 1), ("dnear", 0, 1), ("dfar", 0, 1),
    ("ffn", 1), ("dfar", 1, 1), ("ring", 0, 0, 2), ("dfar", 1, 0), ("dnear", 1, 1), ("comb", 6),
    ("dnear", 1, 0), ("near", 0, 1), ("comb", 7), ("ring", 0, 0, 3), ("fwd", 1, 1), ("fwd", 0, 1),
    ("near", 1, 1), ("fwd", 1, 0), ("near", 1, 0), ("ring", 0, 0, 4), ("coll", 1, 1), ("coll", 0, 1),
    ("ring", 0, 0, 5), ("coll", 1, 0),
)
PARTS = 1
VMEM_LIMIT = 52 * 1024 * 1024
COMBINE_LIMIT = 20 * 1024 * 1024


def _exchange_kernel(dims, len_ref, scale_ref, phi_ref, tok_ref, win_ref, wout_ref, comb_ref, gat_ref,
                     xbuf, xnbuf, phi_in, phi_ring, phi_comb, part, pin, chip, cbuf, rbuf, hsend, hrecv, zpart, zpin, zchip, zrecv,
                     slot_in, by_expert, win, wout, ypart, wbuf,
                     x_sem, phi_sem, w_sem, pr_send, pr_recv, zp_sem, z_sem, relay_recv, hop_recv, fin_recv, hfin_recv, rs_send,
                     ag_recv, ag_send, pg_recv):
    rows, toks, width, slots, seq, experts = dims
    chips = seq // CORES
    own = slots // seq
    per = own // experts
    groups = rows // GROUP_ROWS
    far = chips // 2
    half_e = experts // HALVES
    ring_groups = RS_PLAN.count("R")
    hs = own // HALVES
    par = slots // CORES

    me = lax.axis_index("seq")
    z = me // CORES
    core = me % CORES
    other = 1 - core
    partner = z * CORES + other

    def chip_at(delta):
        return (z + delta + chips) % chips

    def dev_at(delta):
        return chip_at(delta) * CORES + core

    def sign(way):
        return 1 if way == UP else -1

    def remote(src, dst, send, recv, dev):
        return pltpu.make_async_remote_copy(
            src_ref=src, dst_ref=dst, send_sem=send, recv_sem=recv, device_id={"seq": dev}, device_id_type=MESH)

    def wait_bytes(ref, sem):
        pltpu.make_async_copy(ref, ref, sem).wait()

    x_parts = {0: pl.ds(0, 1), 1: pl.ds(1, 1), 2: pl.ds(2, 2), 4: pl.ds(4, rows - 4)}
    x_copies = {b: pltpu.make_async_copy(tok_ref.at[p], xbuf.at[p], x_sem.at[i]) for i, (b, p) in enumerate(x_parts.items())}
    phi_copy = pltpu.make_async_copy(phi_ref, phi_in, phi_sem)
    phi_copy.start()
    x_copies[0].start()
    x_copies[1].start()

    barrier = pltpu.get_barrier_semaphore()
    for delta in range(1, chips):
        pl.semaphore_signal(barrier, inc=1, device_id={"seq": dev_at(delta)}, device_id_type=MESH)
    pl.semaphore_signal(barrier, inc=1, device_id={"seq": partner}, device_id_type=MESH)

    n0 = lax.broadcasted_iota(jnp.int32, (slots, slots), 0)
    n1 = lax.broadcasted_iota(jnp.int32, (slots, slots), 1)
    ring_src = ((n0 % par) // own * CORES + n0 // par) * own + n0 % own
    comb_src = (n0 % (seq * hs)) // hs * own + n0 // (seq * hs) * hs + n0 % hs
    ring_hot = jnp.where(n1 == ring_src, 1.0, 0.0).astype(BF16)
    comb_hot = jnp.where(n1 == comb_src, 1.0, 0.0).astype(BF16)
    gain = scale_ref[0]
    with jax.named_scope("phiwait"):
        phi_copy.wait()
    x_copies[2].start()
    x_copies[4].start()
    params = phi_in[...].astype(F32)
    col_inv = lax.rsqrt(jnp.sum(params * params, axis=0, keepdims=True) + 1e-6)
    phi_norm = (params * (gain * col_inv)).astype(BF16)
    phi_ring[...] = lax.dot_general(ring_hot, phi_norm, NT, preferred_element_type=F32).astype(BF16)
    phi_comb[...] = lax.dot_general(comb_hot, phi_norm, NT, preferred_element_type=F32).astype(BF16)
    bound = gain * 1.01
    zlane = lax.broadcasted_iota(jnp.int32, (slots, 128), 1)
    zpart[...] = jnp.zeros_like(zpart)

    def normalize_part(b, ts):
        xf = xbuf[b, ts].astype(F32)
        inv = lax.rsqrt(jnp.sum(xf * xf, axis=-1, keepdims=True) + 1e-6)
        xnbuf[b, ts] = (xf * inv).astype(BF16)

    def dispatch_stage(r):
        tile = toks // PARTS
        zs = jnp.zeros((slots, 128), F32)
        cut = -(-width // (256 * PARTS)) * 256
        for c in range(PARTS):
            ts = pl.ds(c * tile, tile)
            if r < rows:
                lt = lax.dot_general(phi_ring[...], xnbuf[r, ts], NT, preferred_element_type=F32)
            if r >= 1:
                lo, hi = min(c * cut, width), min((c + 1) * cut, width)
                if lo < hi:
                    s = jnp.dot(wbuf[(r - 1) % 2], xbuf[r - 1, :, lo:hi], preferred_element_type=F32).astype(BF16)
                    for p in range(CORES):
                        part[p, r - 1, :, :, lo:hi] = s[p * par:(p + 1) * par].reshape(chips, own, hi - lo)
            if r + 1 < rows:
                normalize_part(r + 1, ts)
            if r < rows:
                pos = me * toks + c * tile + lax.broadcasted_iota(jnp.int32, (1, tile), 1)
                w = jnp.exp(lt - jnp.where(pos < len_ref[r], bound, 1e30))
                for i in range(tile // 128):
                    zs = zs + w[:, i * 128:(i + 1) * 128]
                wbuf[r % 2, :, ts] = w.astype(BF16)
        if r < rows:
            zsum = jnp.sum(zs, axis=1, keepdims=True)
            hit = jnp.where(zlane == r, zsum, zpart[...].reshape(slots, 128))
            zpart[...] = hit.reshape(CORES, par, 128)

    def combine_row(b):
        logits = lax.dot_general(xnbuf[b], phi_comb[...], NT, preferred_element_type=F32)
        e = jnp.exp(logits)
        total = jnp.sum(e, axis=-1, keepdims=True)
        comb_ref[b] = (e * (1.0 / total)).astype(BF16)

    def span(g):
        return pl.ds(g * GROUP_ROWS, GROUP_ROWS)

    def pair_copy(g):
        return remote(part.at[other, span(g)], pin.at[span(g)], pr_send, pr_recv.at[g], partner)

    def zpair_copy():
        return remote(zpart.at[other], zpin, zp_sem.at[0], zp_sem.at[1], partner)

    def chip_sum(g):
        pair_copy(g).wait_recv()
        chip[span(g)] = (part[core, span(g)].astype(F32) + pin[span(g)].astype(F32)).astype(BF16)

    def is_far(way, index):
        return (index % 2 == 0) == (way == UP)

    def last_of(way, index):
        return far if is_far(way, index) else far - 1

    def hop(g, step):
        for way in (UP, DOWN):
            s = sign(way)
            k = last_of(way, g) - step
            if k < 1:
                continue
            if step == 0:
                src = chip.at[span(g), chip_at(s * k)]
            else:
                with jax.named_scope(f"hop{g}_{step}_{way}"):
                    wait_bytes(hrecv.at[way, k + 1, span(g)], hop_recv.at[way, g, k - 1])
                total = chip[span(g), chip_at(s * k)].astype(F32) + hrecv[way, k + 1, span(g)].astype(F32)
                hsend[way, k, span(g)] = total.astype(BF16)
                src = hsend.at[way, k, span(g)]
            recv = hfin_recv if k == 1 else hop_recv.at[way, g, k - 2]
            remote(src, hrecv.at[way, k, span(g)], rs_send, recv, dev_at(s)).start()

    def late(g):
        return pl.ds((g - ring_groups) * GROUP_ROWS, GROUP_ROWS)

    def rs_first(g):
        for way in (UP, DOWN):
            s = sign(way)
            relay = relay_recv.at[way, g - ring_groups]
            if is_far(way, g):
                remote(chip.at[span(g), chip_at(far * s)], rbuf.at[way, 0, late(g)], rs_send, relay, dev_at(2 * s)).start()
            remote(chip.at[span(g), chip_at(3 * s)], rbuf.at[way, 1, late(g)], rs_send, relay, dev_at(s)).start()
        for way in (UP, DOWN):
            s = sign(way)
            remote(chip.at[span(g), chip_at(s)], rbuf.at[way, 3, late(g)], rs_send, fin_recv, dev_at(s)).start()

    def rs_relay(g):
        for way in (UP, DOWN):
            s = sign(way)
            first = 0 if is_far(way, g) else 1
            with jax.named_scope(f"relay{g}_{way}"):
                wait_bytes(rbuf.at[way, pl.ds(first, 2 - first), late(g)], relay_recv.at[way, g - ring_groups])
            total = chip[span(g), chip_at(2 * s)].astype(F32)
            for kind in range(first, 2):
                total = total + rbuf[way, kind, late(g)].astype(F32)
            cbuf[way, late(g)] = total.astype(BF16)
            remote(cbuf.at[way, late(g)], rbuf.at[way, 2, late(g)], rs_send, fin_recv, dev_at(2 * s)).start()

    def z_exchange():
        zpair_copy().wait_recv()
        zs = zpart[core] + zpin[...]
        zl = lax.broadcasted_iota(jnp.int32, zs.shape, 1)
        hi = zs.astype(BF16).astype(F32)
        mid = (zs - hi).astype(BF16).astype(F32)
        low = zs - hi - mid
        split = jnp.where(zl < rows, hi, 0.0)
        split = split + jnp.where((zl >= rows) & (zl < 2 * rows), pltpu.roll(mid, rows, 1), 0.0)
        split = split + jnp.where((zl >= 2 * rows) & (zl < 3 * rows), pltpu.roll(low, 2 * rows, 1), 0.0)
        zchip[...] = split.astype(BF16).reshape(zchip.shape)
        for delta in range(1, chips):
            remote(zchip.at[chip_at(delta)], zrecv.at[delta], z_sem.at[0], z_sem.at[1], dev_at(delta)).start()

    def weights(h):
        es = pl.ds(h * half_e, half_e)
        return (pltpu.make_async_copy(win_ref.at[es], win.at[es], w_sem.at[h]),
                pltpu.make_async_copy(wout_ref.at[es], wout.at[es], w_sem.at[h]))

    def disp(b):
        if b + 1 in x_parts:
            with jax.named_scope(f"x{b + 1}"):
                x_copies[b + 1].wait()
        with jax.named_scope(f"disp{b}"):
            dispatch_stage(b)
        if b == 1:
            for h in range(HALVES):
                for copy in weights(h):
                    copy.start()

    def comb(b):
        with jax.named_scope(f"comb{b}"):
            combine_row(b)

    def total(g):
        with jax.named_scope(f"sum{g}"):
            chip_sum(g)

    def greet():
        with jax.named_scope("barrier"):
            pl.semaphore_wait(barrier, chips)

    count = rows * own
    i0 = lax.broadcasted_iota(jnp.int32, (count, count), 0)
    i1 = lax.broadcasted_iota(jnp.int32, (count, count), 1)
    rb = rows * per
    src = ((i0 % rb) // per) * own + (i0 // rb) * per + i0 % per
    perm = jnp.where(i1 == src, 1.0, 0.0).astype(BF16)
    hc = half_e * rb
    j0 = lax.broadcasted_iota(jnp.int32, (hc, hc), 0)
    j1 = lax.broadcasted_iota(jnp.int32, (hc, hc), 1)
    back = ((j0 % hs) // per) * rb + (j0 // hs) * per + j0 % per
    unperm = jnp.where(j1 == back, 1.0, 0.0).astype(BF16)

    def own_inputs():
        with jax.named_scope("zwait"):
            wait_bytes(zrecv.at[pl.ds(1, chips - 1)], z_sem.at[1])
        zsum = zchip[z].astype(F32)
        for delta in range(1, chips):
            zsum = zsum + zrecv[delta].astype(F32)
        lane = lax.broadcasted_iota(jnp.int32, zsum.shape, 1)
        if ring_groups:
            with jax.named_scope("hfin"):
                wait_bytes(hrecv.at[:, 1], hfin_recv)
        with jax.named_scope("fin"):
            wait_bytes(rbuf.at[:, pl.ds(2, 2)], fin_recv)
        for b in range(rows):
            s = chip[b, z].astype(F32)
            for way in (UP, DOWN):
                if b < ring_groups * GROUP_ROWS:
                    s = s + hrecv[way, 1, b].astype(F32)
                else:
                    lb = b - ring_groups * GROUP_ROWS
                    s = s + (rbuf[way, 2, lb].astype(F32) + rbuf[way, 3, lb].astype(F32))
            mine = (lane % rows == b) & (lane < 3 * rows)
            zb = jnp.sum(jnp.where(mine, zsum, 0.0), axis=-1, keepdims=True)
            slot_in[b * own:(b + 1) * own] = (s / zb).astype(BF16)
        by_expert[...] = jnp.dot(perm, slot_in[...], preferred_element_type=F32).astype(BF16)

    crows = rows // CHUNKS

    def block(h, c, delta):
        return gat_ref.at[pl.ds(c * crows, crows), h, dev_at(delta)]

    def send(h, c, delta, way, kind, to):
        remote(block(h, c, delta), block(h, c, delta), ag_send, ag_recv.at[h, c, way, kind], dev_at(to)).start()

    def arrived(h, c, way, kind):
        with jax.named_scope(f"ag_h{h}_c{c}_w{way}_k{kind}"):
            wait_bytes(block(h, c, 0), ag_recv.at[h, c, way, kind])

    def publish(h, c, delta):
        remote(block(h, c, delta), block(h, c, delta), ag_send, pg_recv, partner).start()

    def ring(h, c, k):
        for way in (UP, DOWN):
            s = sign(way)
            last = last_of(way, c)
            if k > 1 and k - 1 <= last:
                arrived(h, c, way, k - 2)
            if k <= last:
                send(h, c, -s * (k - 1), way, k - 1, s)
            if k > 1 and k - 1 <= last:
                publish(h, c, -s * (k - 1))
        if k == 1:
            publish(h, c, 0)

    def direct_far(h, c):
        for way in (UP, DOWN):
            send(h, c, 0, way, 1, 2 * sign(way))

    def direct_near(h, c):
        for way in (UP, DOWN):
            send(h, c, 0, way, 0, sign(way))
        publish(h, c, 0)

    def forward(h, c):
        for way in (UP, DOWN):
            s = sign(way)
            arrived(h, c, way, 1)
            if is_far(way, c):
                send(h, c, -2 * s, way, 3, 2 * s)
            send(h, c, -2 * s, way, 2, s)
            publish(h, c, -2 * s)

    def near(h, c):
        for way in (UP, DOWN):
            arrived(h, c, way, 0)
            publish(h, c, -sign(way))

    def collect(h, c):
        for way in (UP, DOWN):
            arrived(h, c, way, 2)
            publish(h, c, -3 * sign(way))
        for way in (UP, DOWN):
            if is_far(way, c):
                arrived(h, c, way, 3)
                publish(h, c, -far * sign(way))

    def expert_half(h):
        with jax.named_scope(f"wwait{h}"):
            wait_bytes(win, w_sem.at[h])
        with jax.named_scope(f"ffn{h}"):
            for i in range(half_e):
                e = h * half_e + i
                hid = jnp.dot(by_expert[e * rb:(e + 1) * rb], win[e], preferred_element_type=F32)
                hid = jax.nn.gelu(hid).astype(BF16)
                ypart[i * rb:(i + 1) * rb] = jnp.dot(hid, wout[e], preferred_element_type=F32).astype(BF16)
            blk = jnp.dot(unperm, ypart[...], preferred_element_type=F32)
            gat_ref[:, h, me] = blk.reshape(rows, hs, width).astype(BF16)

    events = {
        "disp": disp, "bar": greet, "pair": lambda g: pair_copy(g).start(), "total": total, "hop": hop, "first": rs_first,
        "relay": rs_relay, "zpair": lambda: zpair_copy().start(), "z": z_exchange, "comb": comb, "FIN": own_inputs,
        "ffn": expert_half, "ring": ring, "dfar": direct_far, "dnear": direct_near, "fwd": forward, "near": near,
        "coll": collect,
    }
    with jax.named_scope("x0"):
        x_copies[0].wait()
    with jax.named_scope("norm0"):
        normalize_part(0, pl.ds(0, toks))
    for event in ORDER:
        events[event[0]](*event[1:])

    with jax.named_scope("end"):
        wait_bytes(gat_ref.at[:, :, pl.ds(0, chips)], pg_recv)
        wait_bytes(gat_ref.at[:, :, pl.ds(0, seq - 1)], ag_send)
        wait_bytes(pin, pr_send)
        zpair_copy().wait_send()
        wait_bytes(zrecv.at[pl.ds(1, chips - 1)], z_sem.at[0])
        wait_bytes(part.at[0, :, pl.ds(0, chips - 1)], rs_send)


def _combine_kernel(len_ref, comb_ref, gat_ref, out_ref, ybuf, y_sem):
    rows, toks, width = ybuf.shape
    pos = lax.axis_index("seq") * toks + lax.broadcasted_iota(jnp.int32, (toks, 1), 0)

    def out_copy(b):
        return pltpu.make_async_copy(ybuf.at[b], out_ref.at[b], y_sem.at[b])

    for b in range(rows):
        acc = jnp.dot(comb_ref[b], gat_ref[b], preferred_element_type=F32)
        ybuf[b] = jnp.where(pos < len_ref[b], acc, 0.0).astype(BF16)
        out_copy(b).start()
    for b in range(rows):
        out_copy(b).wait()


def solution(mesh):
    seq = mesh.shape["seq"]

    def shard_body(tok, lens, params, scale, w_in, w_out):
        rows, toks, width = tok.shape
        slots = params.shape[1]
        experts, _, ff = w_in.shape
        own = slots // seq
        chips = seq // CORES
        groups = rows // GROUP_ROWS
        ring_groups = RS_PLAN.count("R")
        ring_rows = ring_groups * GROUP_ROWS
        hop_rows = max(ring_rows, 1)
        far = chips // 2
        hs = own // HALVES
        par = slots // CORES
        count = rows * own
        dims = (rows, toks, width, slots, seq, experts)
        dma = pltpu.SemaphoreType.DMA
        any_spec = pl.BlockSpec(memory_space=pl.ANY)
        smem = pl.BlockSpec(memory_space=pltpu.SMEM)
        vmem = pl.BlockSpec(memory_space=pltpu.VMEM)
        comb, gat = pl.pallas_call(
            functools.partial(_exchange_kernel, dims),
            out_shape=(pltpu.VMEM((rows, toks, slots), BF16),
                       pltpu.VMEM((rows, HALVES, seq, hs, width), BF16)),
            in_specs=[smem, smem, any_spec, any_spec, any_spec, any_spec],
            out_specs=(vmem, vmem),
            scratch_shapes=[
                pltpu.VMEM((rows, toks, width), BF16),
                pltpu.VMEM((rows, toks, width), BF16),
                pltpu.VMEM((width, slots), BF16),
                pltpu.VMEM((slots, width), BF16),
                pltpu.VMEM((slots, width), BF16),
                pltpu.VMEM((CORES, rows, chips, own, width), BF16),
                pltpu.VMEM((rows, chips, own, width), BF16),
                pltpu.VMEM((rows, chips, own, width), BF16),
                pltpu.VMEM((2, rows - ring_rows, own, width), BF16),
                pltpu.VMEM((2, 4, rows - ring_rows, own, width), BF16),
                pltpu.VMEM((2, far, hop_rows, own, width), BF16),
                pltpu.VMEM((2, far + 1, hop_rows, own, width), BF16),
                pltpu.VMEM((CORES, par, 128), F32),
                pltpu.VMEM((par, 128), F32),
                pltpu.VMEM((chips, own, 128), BF16),
                pltpu.VMEM((chips, own, 128), BF16),
                pltpu.VMEM((count, width), BF16),
                pltpu.VMEM((count, width), BF16),
                pltpu.VMEM((experts, width, ff), BF16),
                pltpu.VMEM((experts, ff, width), BF16),
                pltpu.VMEM((count // HALVES, width), BF16),
                pltpu.VMEM((2, slots, toks), BF16),
                dma((4,)), dma, dma((HALVES,)), dma, dma((groups,)), dma((2,)), dma((2,)),
                dma((2, groups - ring_groups)), dma((2, max(ring_groups, 1), far - 1)), dma, dma, dma,
                dma((HALVES, CHUNKS, 2, 4)), dma, dma,
            ],
            compiler_params=pltpu.CompilerParams(
                collective_id=0, has_side_effects=True, vmem_limit_bytes=VMEM_LIMIT),
            name="exchange",
        )(lens, scale, params, tok, w_in, w_out)
        gat = gat.reshape(rows, slots, width)
        return pl.pallas_call(
            _combine_kernel,
            out_shape=jax.ShapeDtypeStruct((rows, toks, width), BF16),
            in_specs=[smem, vmem, vmem],
            out_specs=any_spec,
            scratch_shapes=[pltpu.VMEM((rows, toks, width), BF16), dma((rows,))],
            compiler_params=pltpu.CompilerParams(vmem_limit_bytes=COMBINE_LIMIT),
            name="combine",
        )(lens, comb, gat)

    return jax.shard_map(
        shard_body,
        mesh=mesh,
        in_specs=(P("data", "seq", None), P("data"), P(None, None), P(None), P("seq", None, None), P("seq", None, None)),
        out_specs=P("data", "seq", None),
        check_vma=False,
    )
```

```python
import functools

import jax
import jax.numpy as jnp
from jax import lax
from jax.experimental import pallas as pl
from jax.experimental.pallas import tpu as pltpu
from jax.sharding import PartitionSpec as P

F32 = jnp.float32
BF16 = jnp.bfloat16
MESH = pl.DeviceIdType.MESH
NT = (((1,), (1,)), ((), ()))
UP, DOWN = 0, 1
GROUP_ROWS = 2
HALVES = 2
CORES = 2
CHUNKS = 2
ORDER = (
    ("disp", 0), ("disp", 1), ("disp", 2), ("bar",), ("pair", 0), ("disp", 3), ("disp", 4), ("total", 0),
    ("first", 0, 0), ("first", 0, 1), ("pair", 1), ("disp", 5), ("total", 1), ("first", 1, 0), ("disp", 6),
    ("first", 1, 1), ("pair", 2), ("disp", 7), ("disp", 8), ("relay", 0, 0), ("pair", 3), ("zpair",),
    ("total", 2), ("first", 2, 0), ("comb", 0), ("first", 2, 1), ("total", 3), ("first", 3, 0), ("z",),
    ("first", 3, 1), ("relay", 1, 0), ("comb", 1), ("comb", 2), ("relay", 2, 0), ("comb", 3), ("relay", 3, 0),
    ("comb", 4), ("comb", 5), ("relay", 0, 1), ("relay", 1, 1), ("relay", 2, 1), ("relay", 3, 1), ("comb", 6),
    ("fin", 0), ("ffn", 0), ("dfar", 0, 0), ("dfar", 0, 1), ("dnear", 0, 1), ("dnear", 0, 0), ("fin", 1),
    ("ffn", 1), ("dfar", 1, 0), ("comb", 7), ("dfar", 1, 1), ("fwd", 0, 1), ("fwd", 0, 0), ("near", 0, 0),
    ("fwd", 1, 0), ("near", 0, 1), ("dnear", 1, 0), ("fwd", 1, 1), ("dnear", 1, 1), ("coll", 1, 0),
    ("coll", 0, 0), ("near", 1, 0), ("coll", 0, 1), ("near", 1, 1), ("coll", 1, 1),
)
PARTS = 1
VMEM_LIMIT = 52 * 1024 * 1024
COMBINE_LIMIT = 20 * 1024 * 1024


def _exchange_kernel(dims, len_ref, scale_ref, phi_ref, tok_ref, win_ref, wout_ref, comb_ref, gat_ref,
                     xbuf, xnbuf, phi_in, phi_ring, phi_comb, part, pin, chip, cbuf, rbuf, zpart, zpin, zchip, zrecv,
                     slot_in, by_expert, win, wout, ypart, wbuf,
                     x_sem, phi_sem, w_sem, pr_send, pr_recv, zp_sem, z_sem, relay_recv, fin_recv, rs_send,
                     ag_recv, ag_send, pg_recv):
    rows, toks, width, slots, seq, experts = dims
    chips = seq // CORES
    own = slots // seq
    per = own // experts
    groups = rows // GROUP_ROWS
    far = chips // 2
    half_e = experts // HALVES
    hs = own // HALVES
    par = slots // CORES

    me = lax.axis_index("seq")
    z = me // CORES
    core = me % CORES
    other = 1 - core
    partner = z * CORES + other

    def chip_at(delta):
        return (z + delta + chips) % chips

    def dev_at(delta):
        return chip_at(delta) * CORES + core

    def sign(way):
        return 1 if way == UP else -1

    def remote(src, dst, send, recv, dev):
        return pltpu.make_async_remote_copy(
            src_ref=src, dst_ref=dst, send_sem=send, recv_sem=recv, device_id={"seq": dev}, device_id_type=MESH)

    def wait_bytes(ref, sem):
        pltpu.make_async_copy(ref, ref, sem).wait()

    x_parts = {0: pl.ds(0, 1), 1: pl.ds(1, 1), 2: pl.ds(2, 2), 4: pl.ds(4, rows - 4)}
    x_copies = {b: pltpu.make_async_copy(tok_ref.at[p], xbuf.at[p], x_sem.at[i]) for i, (b, p) in enumerate(x_parts.items())}
    phi_copy = pltpu.make_async_copy(phi_ref, phi_in, phi_sem)
    phi_copy.start()
    x_copies[0].start()
    x_copies[1].start()

    barrier = pltpu.get_barrier_semaphore()
    for delta in range(1, chips):
        pl.semaphore_signal(barrier, inc=1, device_id={"seq": dev_at(delta)}, device_id_type=MESH)
    pl.semaphore_signal(barrier, inc=1, device_id={"seq": partner}, device_id_type=MESH)

    n0 = lax.broadcasted_iota(jnp.int32, (slots, slots), 0)
    n1 = lax.broadcasted_iota(jnp.int32, (slots, slots), 1)
    ring_src = ((n0 % (par // HALVES)) // hs * CORES + n0 // par) * own + (n0 % par) // (par // HALVES) * hs + n0 % hs
    comb_src = (n0 % (seq * hs)) // hs * own + n0 // (seq * hs) * hs + n0 % hs
    ring_hot = jnp.where(n1 == ring_src, 1.0, 0.0).astype(BF16)
    comb_hot = jnp.where(n1 == comb_src, 1.0, 0.0).astype(BF16)
    gain = scale_ref[0]
    with jax.named_scope("phiwait"):
        phi_copy.wait()
    x_copies[2].start()
    x_copies[4].start()
    params = phi_in[...].astype(F32)
    col_inv = lax.rsqrt(jnp.sum(params * params, axis=0, keepdims=True) + 1e-6)
    phi_norm = (params * (gain * col_inv)).astype(BF16)
    phi_ring[...] = lax.dot_general(ring_hot, phi_norm, NT, preferred_element_type=F32).astype(BF16)
    phi_comb[...] = lax.dot_general(comb_hot, phi_norm, NT, preferred_element_type=F32).astype(BF16)
    bound = gain * 1.01
    zlane = lax.broadcasted_iota(jnp.int32, (slots, 128), 1)
    zpart[...] = jnp.zeros_like(zpart)

    def normalize_part(b, ts):
        xf = xbuf[b, ts].astype(F32)
        inv = lax.rsqrt(jnp.sum(xf * xf, axis=-1, keepdims=True) + 1e-6)
        xnbuf[b, ts] = (xf * inv).astype(BF16)

    def dispatch_stage(r):
        tile = toks // PARTS
        zs = jnp.zeros((slots, 128), F32)
        cut = -(-width // (256 * PARTS)) * 256
        for c in range(PARTS):
            ts = pl.ds(c * tile, tile)
            if r < rows:
                lt = lax.dot_general(phi_ring[...], xnbuf[r, ts], NT, preferred_element_type=F32)
            if r >= 1:
                lo, hi = min(c * cut, width), min((c + 1) * cut, width)
                if lo < hi:
                    s = jnp.dot(wbuf[(r - 1) % 2], xbuf[r - 1, :, lo:hi], preferred_element_type=F32).astype(BF16)
                    for p in range(CORES):
                        part[p, r - 1, :, :, :, lo:hi] = s[p * par:(p + 1) * par].reshape(HALVES, chips, hs, hi - lo)
            if r + 1 < rows:
                normalize_part(r + 1, ts)
            if r < rows:
                pos = me * toks + c * tile + lax.broadcasted_iota(jnp.int32, (1, tile), 1)
                w = jnp.exp(lt - jnp.where(pos < len_ref[r], bound, 1e30))
                for i in range(tile // 128):
                    zs = zs + w[:, i * 128:(i + 1) * 128]
                wbuf[r % 2, :, ts] = w.astype(BF16)
        if r < rows:
            zsum = jnp.sum(zs, axis=1, keepdims=True)
            hit = jnp.where(zlane == r, zsum, zpart[...].reshape(slots, 128))
            zpart[...] = hit.reshape(CORES, par, 128)

    def combine_row(b):
        logits = lax.dot_general(xnbuf[b], phi_comb[...], NT, preferred_element_type=F32)
        e = jnp.exp(logits)
        total = jnp.sum(e, axis=-1, keepdims=True)
        comb_ref[b] = (e * (1.0 / total)).astype(BF16)

    def span(g):
        return pl.ds(g * GROUP_ROWS, GROUP_ROWS)

    def pair_copy(g):
        return remote(part.at[other, span(g)], pin.at[span(g)], pr_send, pr_recv.at[g], partner)

    def zpair_copy():
        return remote(zpart.at[other], zpin, zp_sem.at[0], zp_sem.at[1], partner)

    def chip_sum(g):
        pair_copy(g).wait_recv()
        chip[span(g)] = (part[core, span(g)].astype(F32) + pin[span(g)].astype(F32)).astype(BF16)

    def is_far(way, index):
        return (index % 2 == 0) == (way == UP)

    def last_of(way, index):
        return far if is_far(way, index) else far - 1

    def rs_first(g, h):
        for way in (UP, DOWN):
            s = sign(way)
            relay = relay_recv.at[way, g, h]
            if is_far(way, g + h):
                remote(chip.at[span(g), h, chip_at(far * s)], rbuf.at[way, 0, h, span(g)], rs_send, relay, dev_at(2 * s)).start()
            remote(chip.at[span(g), h, chip_at(3 * s)], rbuf.at[way, 1, h, span(g)], rs_send, relay, dev_at(s)).start()
        for way in (UP, DOWN):
            s = sign(way)
            remote(chip.at[span(g), h, chip_at(s)], rbuf.at[way, 3, h, span(g)], rs_send, fin_recv.at[h], dev_at(s)).start()

    def rs_relay(g, h):
        for way in (UP, DOWN):
            s = sign(way)
            first = 0 if is_far(way, g + h) else 1
            with jax.named_scope(f"relay{g}_{h}_{way}"):
                wait_bytes(rbuf.at[way, pl.ds(first, 2 - first), h, span(g)], relay_recv.at[way, g, h])
            total = chip[span(g), h, chip_at(2 * s)].astype(F32)
            for kind in range(first, 2):
                total = total + rbuf[way, kind, h, span(g)].astype(F32)
            cbuf[way, h, span(g)] = total.astype(BF16)
            remote(cbuf.at[way, h, span(g)], rbuf.at[way, 2, h, span(g)], rs_send, fin_recv.at[h], dev_at(2 * s)).start()

    def z_exchange():
        zpair_copy().wait_recv()
        zs = zpart[core] + zpin[...]
        zl = lax.broadcasted_iota(jnp.int32, zs.shape, 1)
        hi = zs.astype(BF16).astype(F32)
        mid = (zs - hi).astype(BF16).astype(F32)
        low = zs - hi - mid
        split = jnp.where(zl < rows, hi, 0.0)
        split = split + jnp.where((zl >= rows) & (zl < 2 * rows), pltpu.roll(mid, rows, 1), 0.0)
        split = split + jnp.where((zl >= 2 * rows) & (zl < 3 * rows), pltpu.roll(low, 2 * rows, 1), 0.0)
        zchip[...] = split.astype(BF16).reshape(zchip.shape)
        for delta in range(1, chips):
            remote(zchip.at[:, chip_at(delta)], zrecv.at[delta], z_sem.at[0], z_sem.at[1], dev_at(delta)).start()

    def weights(h):
        es = pl.ds(h * half_e, half_e)
        return (pltpu.make_async_copy(win_ref.at[es], win.at[es], w_sem.at[h]),
                pltpu.make_async_copy(wout_ref.at[es], wout.at[es], w_sem.at[h]))

    def disp(b):
        if b + 1 in x_parts:
            with jax.named_scope(f"x{b + 1}"):
                x_copies[b + 1].wait()
        with jax.named_scope(f"disp{b}"):
            dispatch_stage(b)
        if b == 1:
            for h in range(HALVES):
                for copy in weights(h):
                    copy.start()

    def comb(b):
        with jax.named_scope(f"comb{b}"):
            combine_row(b)

    def total(g):
        with jax.named_scope(f"sum{g}"):
            chip_sum(g)

    def greet():
        with jax.named_scope("barrier"):
            pl.semaphore_wait(barrier, chips)

    rb = rows * per
    hc = half_e * rb
    j0 = lax.broadcasted_iota(jnp.int32, (hc, hc), 0)
    j1 = lax.broadcasted_iota(jnp.int32, (hc, hc), 1)
    back = ((j0 % hs) // per) * rb + (j0 // hs) * per + j0 % per
    unperm = jnp.where(j1 == back, 1.0, 0.0).astype(BF16)
    src = ((j0 % rb) // per) * hs + (j0 // rb) * per + j0 % per
    perm = jnp.where(j1 == src, 1.0, 0.0).astype(BF16)

    def own_inputs(h):
        if h == 0:
            with jax.named_scope("zwait"):
                wait_bytes(zrecv.at[pl.ds(1, chips - 1)], z_sem.at[1])
        zsum = zchip[h, z].astype(F32)
        for delta in range(1, chips):
            zsum = zsum + zrecv[delta, h].astype(F32)
        lane = lax.broadcasted_iota(jnp.int32, zsum.shape, 1)
        with jax.named_scope(f"fin{h}"):
            wait_bytes(rbuf.at[:, pl.ds(2, 2), h], fin_recv.at[h])
        for b in range(rows):
            s = chip[b, h, z].astype(F32)
            for way in (UP, DOWN):
                s = s + (rbuf[way, 2, h, b].astype(F32) + rbuf[way, 3, h, b].astype(F32))
            mine = (lane % rows == b) & (lane < 3 * rows)
            zb = jnp.sum(jnp.where(mine, zsum, 0.0), axis=-1, keepdims=True)
            slot_in[h, b] = s / zb
        inputs = slot_in[h].reshape(rows * hs, width).astype(BF16)
        by_expert[h] = jnp.dot(perm, inputs, preferred_element_type=F32).astype(BF16)

    crows = rows // CHUNKS

    def block(h, c, delta):
        return gat_ref.at[pl.ds(c * crows, crows), h, dev_at(delta)]

    def send(h, c, delta, way, kind, to):
        remote(block(h, c, delta), block(h, c, delta), ag_send, ag_recv.at[h, c, way, kind], dev_at(to)).start()

    def arrived(h, c, way, kind):
        with jax.named_scope(f"ag_h{h}_c{c}_w{way}_k{kind}"):
            wait_bytes(block(h, c, 0), ag_recv.at[h, c, way, kind])

    def publish(h, c, delta):
        remote(block(h, c, delta), block(h, c, delta), ag_send, pg_recv, partner).start()

    def ring(h, c, k):
        for way in (UP, DOWN):
            s = sign(way)
            last = last_of(way, c)
            if k > 1 and k - 1 <= last:
                arrived(h, c, way, k - 2)
            if k <= last:
                send(h, c, -s * (k - 1), way, k - 1, s)
            if k > 1 and k - 1 <= last:
                publish(h, c, -s * (k - 1))
        if k == 1:
            publish(h, c, 0)

    def direct_far(h, c):
        for way in (UP, DOWN):
            send(h, c, 0, way, 1, 2 * sign(way))

    def direct_near(h, c):
        for way in (UP, DOWN):
            send(h, c, 0, way, 0, sign(way))
        publish(h, c, 0)

    def forward(h, c):
        for way in (UP, DOWN):
            s = sign(way)
            arrived(h, c, way, 1)
            if is_far(way, c):
                send(h, c, -2 * s, way, 3, 2 * s)
            send(h, c, -2 * s, way, 2, s)
            publish(h, c, -2 * s)

    def near(h, c):
        for way in (UP, DOWN):
            arrived(h, c, way, 0)
            publish(h, c, -sign(way))

    def collect(h, c):
        for way in (UP, DOWN):
            arrived(h, c, way, 2)
            publish(h, c, -3 * sign(way))
        for way in (UP, DOWN):
            if is_far(way, c):
                arrived(h, c, way, 3)
                publish(h, c, -far * sign(way))

    def expert_half(h):
        with jax.named_scope(f"wwait{h}"):
            wait_bytes(win, w_sem.at[h])
        with jax.named_scope(f"ffn{h}"):
            for i in range(half_e):
                e = h * half_e + i
                hid = jnp.dot(by_expert[h, i * rb:(i + 1) * rb], win[e], preferred_element_type=F32)
                hid = jax.nn.gelu(hid).astype(BF16)
                ypart[i * rb:(i + 1) * rb] = jnp.dot(hid, wout[e], preferred_element_type=F32).astype(BF16)
            blk = jnp.dot(unperm, ypart[...], preferred_element_type=F32)
            gat_ref[:, h, me] = blk.reshape(rows, hs, width).astype(BF16)

    events = {
        "disp": disp, "bar": greet, "pair": lambda g: pair_copy(g).start(), "total": total, "first": rs_first,
        "relay": rs_relay, "zpair": lambda: zpair_copy().start(), "z": z_exchange, "comb": comb, "fin": own_inputs,
        "ffn": expert_half, "ring": ring, "dfar": direct_far, "dnear": direct_near, "fwd": forward, "near": near,
        "coll": collect,
    }
    with jax.named_scope("x0"):
        x_copies[0].wait()
    with jax.named_scope("norm0"):
        normalize_part(0, pl.ds(0, toks))
    for event in ORDER:
        events[event[0]](*event[1:])

    with jax.named_scope("end"):
        wait_bytes(gat_ref.at[:, :, pl.ds(0, chips)], pg_recv)
        wait_bytes(gat_ref.at[:, :, pl.ds(0, seq - 1)], ag_send)
        wait_bytes(pin, pr_send)
        zpair_copy().wait_send()
        wait_bytes(zrecv.at[pl.ds(1, chips - 1)], z_sem.at[0])
        wait_bytes(part.at[0, :, :, pl.ds(0, chips - 1)], rs_send)


def _combine_kernel(len_ref, comb_ref, gat_ref, out_ref, ybuf, y_sem):
    rows, toks, width = ybuf.shape
    pos = lax.axis_index("seq") * toks + lax.broadcasted_iota(jnp.int32, (toks, 1), 0)

    def out_copy(b):
        return pltpu.make_async_copy(ybuf.at[b], out_ref.at[b], y_sem.at[b])

    for b in range(rows):
        acc = jnp.dot(comb_ref[b], gat_ref[b], preferred_element_type=F32)
        ybuf[b] = jnp.where(pos < len_ref[b], acc, 0.0).astype(BF16)
        out_copy(b).start()
    for b in range(rows):
        out_copy(b).wait()


def solution(mesh):
    seq = mesh.shape["seq"]

    def shard_body(tok, lens, params, scale, w_in, w_out):
        rows, toks, width = tok.shape
        slots = params.shape[1]
        experts, _, ff = w_in.shape
        own = slots // seq
        chips = seq // CORES
        groups = rows // GROUP_ROWS
        far = chips // 2
        hs = own // HALVES
        par = slots // CORES
        count = rows * own
        dims = (rows, toks, width, slots, seq, experts)
        dma = pltpu.SemaphoreType.DMA
        any_spec = pl.BlockSpec(memory_space=pl.ANY)
        smem = pl.BlockSpec(memory_space=pltpu.SMEM)
        vmem = pl.BlockSpec(memory_space=pltpu.VMEM)
        comb, gat = pl.pallas_call(
            functools.partial(_exchange_kernel, dims),
            out_shape=(pltpu.VMEM((rows, toks, slots), BF16),
                       pltpu.VMEM((rows, HALVES, seq, hs, width), BF16)),
            in_specs=[smem, smem, any_spec, any_spec, any_spec, any_spec],
            out_specs=(vmem, vmem),
            scratch_shapes=[
                pltpu.VMEM((rows, toks, width), BF16),
                pltpu.VMEM((rows, toks, width), BF16),
                pltpu.VMEM((width, slots), BF16),
                pltpu.VMEM((slots, width), BF16),
                pltpu.VMEM((slots, width), BF16),
                pltpu.VMEM((CORES, rows, HALVES, chips, hs, width), BF16),
                pltpu.VMEM((rows, HALVES, chips, hs, width), BF16),
                pltpu.VMEM((rows, HALVES, chips, hs, width), BF16),
                pltpu.VMEM((2, HALVES, rows, hs, width), BF16),
                pltpu.VMEM((2, 4, HALVES, rows, hs, width), BF16),
                pltpu.VMEM((CORES, par, 128), F32),
                pltpu.VMEM((par, 128), F32),
                pltpu.VMEM((HALVES, chips, hs, 128), BF16),
                pltpu.VMEM((chips, HALVES, hs, 128), BF16),
                pltpu.VMEM((HALVES, rows, hs, width), F32),
                pltpu.VMEM((HALVES, count // HALVES, width), BF16),
                pltpu.VMEM((experts, width, ff), BF16),
                pltpu.VMEM((experts, ff, width), BF16),
                pltpu.VMEM((count // HALVES, width), BF16),
                pltpu.VMEM((2, slots, toks), BF16),
                dma((4,)), dma, dma((HALVES,)), dma, dma((groups,)), dma((2,)), dma((2,)),
                dma((2, groups, HALVES)), dma((HALVES,)), dma,
                dma((HALVES, CHUNKS, 2, 4)), dma, dma,
            ],
            compiler_params=pltpu.CompilerParams(
                collective_id=0, has_side_effects=True, vmem_limit_bytes=VMEM_LIMIT),
            name="exchange",
        )(lens, scale, params, tok, w_in, w_out)
        gat = gat.reshape(rows, slots, width)
        return pl.pallas_call(
            _combine_kernel,
            out_shape=jax.ShapeDtypeStruct((rows, toks, width), BF16),
            in_specs=[smem, vmem, vmem],
            out_specs=any_spec,
            scratch_shapes=[pltpu.VMEM((rows, toks, width), BF16), dma((rows,))],
            compiler_params=pltpu.CompilerParams(vmem_limit_bytes=COMBINE_LIMIT),
            name="combine",
        )(lens, comb, gat)

    return jax.shard_map(
        shard_body,
        mesh=mesh,
        in_specs=(P("data", "seq", None), P("data"), P(None, None), P(None), P("seq", None, None), P("seq", None, None)),
        out_specs=P("data", "seq", None),
        check_vma=False,
    )
```

```python
import functools

import jax
import jax.numpy as jnp
from jax import lax
from jax.experimental import pallas as pl
from jax.experimental.pallas import tpu as pltpu
from jax.sharding import PartitionSpec as P

F32 = jnp.float32
BF16 = jnp.bfloat16
MESH = pl.DeviceIdType.MESH
NT = (((1,), (1,)), ((), ()))
UP, DOWN = 0, 1
GROUP_ROWS = 2
HALVES = 2
CORES = 2
CHUNKS = 2
ORDER = (
    ("disp", 0), ("disp", 1), ("disp", 2), ("bar",), ("pair", 0), ("disp", 3), ("disp", 4), ("total", 0),
    ("pair", 1), ("first", 0, 0), ("disp", 5), ("first", 0, 1), ("disp", 6), ("total", 1), ("first", 1, 1),
    ("pair", 2), ("first", 1, 0), ("disp", 7), ("disp", 8), ("total", 2), ("pair", 3), ("zpair",),
    ("first", 2, 0), ("relay", 0, 0), ("comb", 0), ("total", 3), ("first", 3, 0), ("first", 3, 1), ("z",),
    ("first", 2, 1), ("comb", 1), ("relay", 1, 0), ("comb", 2), ("relay", 2, 0), ("comb", 3), ("relay", 3, 0),
    ("comb", 4), ("comb", 5), ("relay", 0, 1), ("comb", 6), ("relay", 1, 1), ("relay", 2, 1), ("relay", 3, 1),
    ("fin", 0), ("ffn", 0), ("dfar", 0, 0), ("dfar", 0, 1), ("dnear", 0, 1), ("fin", 1), ("dnear", 0, 0),
    ("ffn", 1), ("dfar", 1, 0), ("dfar", 1, 1), ("near", 0, 0), ("fwd", 0, 0), ("fwd", 0, 1), ("near", 0, 1),
    ("fwd", 1, 0), ("dnear", 1, 1), ("fwd", 1, 1), ("dnear", 1, 0), ("coll", 0, 0), ("comb", 7),
    ("coll", 1, 0), ("near", 1, 1), ("coll", 0, 1), ("coll", 1, 1), ("near", 1, 0),
)
PARTS = 2
VMEM_LIMIT = 52 * 1024 * 1024
COMBINE_LIMIT = 20 * 1024 * 1024


def _exchange_kernel(dims, len_hbm, scale_ref, phi_ref, tok_ref, win_ref, wout_ref, comb_ref, gat_ref, lens_ref,
                     len_ref, xbuf, xnbuf, phi_in, phi_ring, phi_comb, part, pin, chip, cbuf, rbuf, zpart, zpin, zchip, zrecv,
                     slot_in, by_expert, win, wout, ypart, wbuf,
                     x_sem, phi_sem, scalar_sem, w_sem, pr_send, pr_recv, zp_sem, z_sem, relay_recv, fin_recv, rs_send,
                     ag_recv, ag_send, pg_recv):
    rows, toks, width, slots, seq, experts = dims
    chips = seq // CORES
    own = slots // seq
    per = own // experts
    groups = rows // GROUP_ROWS
    far = chips // 2
    half_e = experts // HALVES
    hs = own // HALVES
    par = slots // CORES

    me = lax.axis_index("seq")
    z = me // CORES
    core = me % CORES
    other = 1 - core
    partner = z * CORES + other

    def chip_at(delta):
        return (z + delta + chips) % chips

    def dev_at(delta):
        return chip_at(delta) * CORES + core

    def sign(way):
        return 1 if way == UP else -1

    def remote(src, dst, send, recv, dev):
        return pltpu.make_async_remote_copy(
            src_ref=src, dst_ref=dst, send_sem=send, recv_sem=recv, device_id={"seq": dev}, device_id_type=MESH)

    def wait_bytes(ref, sem):
        pltpu.make_async_copy(ref, ref, sem).wait()

    x_parts = {0: pl.ds(0, 1), 1: pl.ds(1, 1), 2: pl.ds(2, 2), 4: pl.ds(4, rows - 4)}
    x_copies = {b: pltpu.make_async_copy(tok_ref.at[p], xbuf.at[p], x_sem.at[i]) for i, (b, p) in enumerate(x_parts.items())}
    phi_copy = pltpu.make_async_copy(phi_ref, phi_in, phi_sem)
    len_copy = pltpu.make_async_copy(len_hbm, len_ref, scalar_sem)
    phi_copy.start()
    len_copy.start()
    x_copies[0].start()
    x_copies[1].start()

    barrier = pltpu.get_barrier_semaphore()
    for delta in range(1, chips):
        pl.semaphore_signal(barrier, inc=1, device_id={"seq": dev_at(delta)}, device_id_type=MESH)
    pl.semaphore_signal(barrier, inc=1, device_id={"seq": partner}, device_id_type=MESH)

    n0 = lax.broadcasted_iota(jnp.int32, (slots, slots), 0)
    n1 = lax.broadcasted_iota(jnp.int32, (slots, slots), 1)
    ring_src = ((n0 % (par // HALVES)) // hs * CORES + n0 // par) * own + (n0 % par) // (par // HALVES) * hs + n0 % hs
    comb_src = (n0 % (seq * hs)) // hs * own + n0 // (seq * hs) * hs + n0 % hs
    ring_hot = jnp.where(n1 == ring_src, 1.0, 0.0).astype(BF16)
    comb_hot = jnp.where(n1 == comb_src, 1.0, 0.0).astype(BF16)
    with jax.named_scope("phiwait"):
        phi_copy.wait()
        len_copy.wait()
    gain = scale_ref[0]
    x_copies[2].start()
    x_copies[4].start()
    params = phi_in[...].astype(F32)
    col_inv = lax.rsqrt(jnp.sum(params * params, axis=0, keepdims=True) + 1e-6)
    phi_norm = (params * (gain * col_inv)).astype(BF16)
    phi_ring[...] = lax.dot_general(ring_hot, phi_norm, NT, preferred_element_type=F32).astype(BF16)
    phi_comb[...] = lax.dot_general(comb_hot, phi_norm, NT, preferred_element_type=F32).astype(BF16)
    bound = gain * 1.01
    zlane = lax.broadcasted_iota(jnp.int32, (slots, 128), 1)
    zpart[...] = jnp.zeros_like(zpart)
    row_id = lax.broadcasted_iota(jnp.int32, lens_ref.shape, 0)
    lens = jnp.zeros(lens_ref.shape, jnp.int32)
    for b in range(rows):
        lens = jnp.where(row_id == b, len_ref[b], lens)
    lens_ref[...] = lens

    def normalize_part(b, ts):
        xf = xbuf[b, ts].astype(F32)
        inv = lax.rsqrt(jnp.sum(xf * xf, axis=-1, keepdims=True) + 1e-6)
        xnbuf[b, ts] = (xf * inv).astype(BF16)

    def weigh(r, ts):
        lt = lax.dot_general(phi_ring[...], xnbuf[r, ts], NT, preferred_element_type=F32)
        pos = me * toks + ts.start + lax.broadcasted_iota(jnp.int32, (1, ts.size), 1)
        w = jnp.exp(lt - jnp.where(pos < len_ref[r], bound, 1e30))
        wbuf[r % 2, :, ts] = w.astype(BF16)
        return sum(w[:, i * 128:(i + 1) * 128] for i in range(ts.size // 128))

    def slot_sums(r, lo, hi):
        s = jnp.dot(wbuf[r % 2], xbuf[r, :, lo:hi], preferred_element_type=F32).astype(BF16)
        for p in range(CORES):
            part[p, r, :, :, :, lo:hi] = s[p * par:(p + 1) * par].reshape(HALVES, chips, hs, hi - lo)

    def dispatch_stage(r):
        tile = toks // PARTS
        zs = jnp.zeros((slots, 128), F32)
        if r >= 1:
            slot_sums(r - 1, 0, width)
        for c in range(PARTS):
            ts = pl.ds(c * tile, tile)
            if r < rows:
                zs = zs + weigh(r, ts)
            if r + 1 < rows:
                normalize_part(r + 1, ts)
        if r < rows:
            zsum = jnp.sum(zs, axis=1, keepdims=True)
            hit = jnp.where(zlane == r, zsum, zpart[...].reshape(slots, 128))
            zpart[...] = hit.reshape(CORES, par, 128)

    def combine_row(b):
        logits = lax.dot_general(xnbuf[b], phi_comb[...], NT, preferred_element_type=F32)
        e = jnp.exp(logits)
        total = jnp.sum(e, axis=-1, keepdims=True)
        comb_ref[b] = (e * (1.0 / total)).astype(BF16)

    def span(g):
        return pl.ds(g * GROUP_ROWS, GROUP_ROWS)

    def pair_copy(g):
        return remote(part.at[other, span(g)], pin.at[span(g)], pr_send, pr_recv.at[g], partner)

    def zpair_copy():
        return remote(zpart.at[other], zpin, zp_sem.at[0], zp_sem.at[1], partner)

    def chip_sum(g):
        pair_copy(g).wait_recv()
        chip[span(g)] = (part[core, span(g)].astype(F32) + pin[span(g)].astype(F32)).astype(BF16)

    def is_far(way, index):
        return (index % 2 == 0) == (way == UP)

    def rs_first(g, h):
        for way in (UP, DOWN):
            s = sign(way)
            relay = relay_recv.at[way, g, h]
            if is_far(way, g + h):
                remote(chip.at[span(g), h, chip_at(far * s)], rbuf.at[way, 0, h, span(g)], rs_send, relay, dev_at(2 * s)).start()
            remote(chip.at[span(g), h, chip_at(3 * s)], rbuf.at[way, 1, h, span(g)], rs_send, relay, dev_at(s)).start()
        for way in (UP, DOWN):
            s = sign(way)
            remote(chip.at[span(g), h, chip_at(s)], rbuf.at[way, 3, h, span(g)], rs_send, fin_recv.at[h], dev_at(s)).start()

    def rs_relay(g, h):
        for way in (UP, DOWN):
            s = sign(way)
            first = 0 if is_far(way, g + h) else 1
            with jax.named_scope(f"relay{g}_{h}_{way}"):
                wait_bytes(rbuf.at[way, pl.ds(first, 2 - first), h, span(g)], relay_recv.at[way, g, h])
            total = chip[span(g), h, chip_at(2 * s)].astype(F32)
            for kind in range(first, 2):
                total = total + rbuf[way, kind, h, span(g)].astype(F32)
            cbuf[way, h, span(g)] = total.astype(BF16)
            remote(cbuf.at[way, h, span(g)], rbuf.at[way, 2, h, span(g)], rs_send, fin_recv.at[h], dev_at(2 * s)).start()

    def z_exchange():
        zpair_copy().wait_recv()
        zs = zpart[core] + zpin[...]
        zl = lax.broadcasted_iota(jnp.int32, zs.shape, 1)
        hi = zs.astype(BF16).astype(F32)
        mid = (zs - hi).astype(BF16).astype(F32)
        low = zs - hi - mid
        split = jnp.where(zl < rows, hi, 0.0)
        split = split + jnp.where((zl >= rows) & (zl < 2 * rows), pltpu.roll(mid, rows, 1), 0.0)
        split = split + jnp.where((zl >= 2 * rows) & (zl < 3 * rows), pltpu.roll(low, 2 * rows, 1), 0.0)
        zchip[...] = split.astype(BF16).reshape(zchip.shape)
        for delta in range(1, chips):
            remote(zchip.at[:, chip_at(delta)], zrecv.at[delta], z_sem.at[0], z_sem.at[1], dev_at(delta)).start()

    def weights(h):
        es = pl.ds(h * half_e, half_e)
        return (pltpu.make_async_copy(win_ref.at[es], win.at[es], w_sem.at[h]),
                pltpu.make_async_copy(wout_ref.at[es], wout.at[es], w_sem.at[h]))

    def disp(b):
        if b + 1 in x_parts:
            with jax.named_scope(f"x{b + 1}"):
                x_copies[b + 1].wait()
        with jax.named_scope(f"disp{b}"):
            dispatch_stage(b)
        if b == 1:
            for h in range(HALVES):
                for copy in weights(h):
                    copy.start()

    def comb(b):
        with jax.named_scope(f"comb{b}"):
            combine_row(b)

    def total(g):
        with jax.named_scope(f"sum{g}"):
            chip_sum(g)

    def greet():
        with jax.named_scope("barrier"):
            pl.semaphore_wait(barrier, chips)

    rb = rows * per
    hc = half_e * rb
    j0 = lax.broadcasted_iota(jnp.int32, (hc, hc), 0)
    j1 = lax.broadcasted_iota(jnp.int32, (hc, hc), 1)
    back = ((j0 % hs) // per) * rb + (j0 // hs) * per + j0 % per
    unperm = jnp.where(j1 == back, 1.0, 0.0).astype(BF16)
    src = ((j0 % rb) // per) * hs + (j0 // rb) * per + j0 % per
    perm = jnp.where(j1 == src, 1.0, 0.0).astype(BF16)

    def own_inputs(h):
        if h == 0:
            with jax.named_scope("zwait"):
                wait_bytes(zrecv.at[pl.ds(1, chips - 1)], z_sem.at[1])
        zsum = zchip[h, z].astype(F32)
        for delta in range(1, chips):
            zsum = zsum + zrecv[delta, h].astype(F32)
        lane = lax.broadcasted_iota(jnp.int32, zsum.shape, 1)
        with jax.named_scope(f"fin{h}"):
            wait_bytes(rbuf.at[:, pl.ds(2, 2), h], fin_recv.at[h])
        for b in range(rows):
            s = chip[b, h, z].astype(F32)
            for way in (UP, DOWN):
                s = s + (rbuf[way, 2, h, b].astype(F32) + rbuf[way, 3, h, b].astype(F32))
            mine = (lane % rows == b) & (lane < 3 * rows)
            zb = jnp.sum(jnp.where(mine, zsum, 0.0), axis=-1, keepdims=True)
            slot_in[h, b] = s / zb
        inputs = slot_in[h].reshape(rows * hs, width).astype(BF16)
        by_expert[h] = jnp.dot(perm, inputs, preferred_element_type=F32).astype(BF16)

    crows = rows // CHUNKS

    def chunk(c):
        return pl.ds(c * crows, crows)

    def send(h, c, delta, sem, to):
        ref = gat_ref.at[chunk(c), h, dev_at(delta)]
        remote(ref, ref, ag_send, ag_recv.at[h, c, sem], dev_at(to)).start()

    def arrived(h, c, sem, count):
        with jax.named_scope(f"ag_h{h}_c{c}_s{sem}"):
            wait_bytes(gat_ref.at[chunk(c), h, pl.ds(0, count)], ag_recv.at[h, c, sem])

    def publish(h, c, delta):
        ref = gat_ref.at[chunk(c), h, dev_at(delta)]
        remote(ref, ref, ag_send, pg_recv.at[c], partner).start()

    def direct_far(h, c):
        for way in (UP, DOWN):
            send(h, c, 0, way, 2 * sign(way))

    def direct_near(h, c):
        for way in (UP, DOWN):
            send(h, c, 0, 2, sign(way))
        publish(h, c, 0)

    def forward(h, c):
        for way in (UP, DOWN):
            s = sign(way)
            arrived(h, c, way, 1)
            if is_far(way, c):
                send(h, c, -2 * s, 3, 2 * s)
            send(h, c, -2 * s, 3, s)
            publish(h, c, -2 * s)

    def near(h, c):
        arrived(h, c, 2, 2)
        publish(h, c, -1)
        publish(h, c, 1)

    def collect(h, c):
        arrived(h, c, 3, 3)
        publish(h, c, -3)
        publish(h, c, 3)
        publish(h, c, -far if is_far(UP, c) else far)

    def expert_half(h):
        with jax.named_scope(f"wwait{h}"):
            wait_bytes(win, w_sem.at[h])
        with jax.named_scope(f"ffn{h}"):
            for i in range(half_e):
                e = h * half_e + i
                hid = jnp.dot(by_expert[h, i * rb:(i + 1) * rb], win[e], preferred_element_type=F32)
                hid = jax.nn.gelu(hid).astype(BF16)
                ypart[i * rb:(i + 1) * rb] = jnp.dot(hid, wout[e], preferred_element_type=F32).astype(BF16)
            blk = jnp.dot(unperm, ypart[...], preferred_element_type=F32)
            gat_ref[:, h, me] = blk.reshape(rows, hs, width).astype(BF16)

    events = {
        "disp": disp, "bar": greet, "pair": lambda g: pair_copy(g).start(), "total": total, "first": rs_first,
        "relay": rs_relay, "zpair": lambda: zpair_copy().start(), "z": z_exchange, "comb": comb, "fin": own_inputs,
        "ffn": expert_half, "dfar": direct_far, "dnear": direct_near, "fwd": forward, "near": near,
        "coll": collect,
    }
    with jax.named_scope("x0"):
        x_copies[0].wait()
    with jax.named_scope("norm0"):
        normalize_part(0, pl.ds(0, toks))
    for event in ORDER:
        events[event[0]](*event[1:])

    with jax.named_scope("end"):
        for c in range(CHUNKS):
            wait_bytes(gat_ref.at[chunk(c), :, pl.ds(0, chips)], pg_recv.at[c])
        wait_bytes(gat_ref.at[:, :, pl.ds(0, seq - 1)], ag_send)
        wait_bytes(pin, pr_send)
        zpair_copy().wait_send()
        wait_bytes(zrecv.at[pl.ds(1, chips - 1)], z_sem.at[0])
        wait_bytes(part.at[0, :, :, pl.ds(0, chips - 1)], rs_send)


def _combine_kernel(reach_ref, comb_ref, gat_ref, out_ref, ybuf, y_sem):
    rows, toks, width = ybuf.shape
    lanes = reach_ref.shape[1]
    pos = lax.axis_index("seq") * toks + lax.broadcasted_iota(jnp.int32, (toks, lanes), 0)

    def out_copy(b):
        return pltpu.make_async_copy(ybuf.at[b], out_ref.at[b], y_sem.at[b])

    for b in range(rows):
        acc = jnp.dot(comb_ref[b], gat_ref[b], preferred_element_type=F32)
        valid = pos < reach_ref[b:b + 1]
        for i in range(width // lanes):
            part = slice(i * lanes, (i + 1) * lanes)
            ybuf[b, :, part] = jnp.where(valid, acc[:, part], 0.0).astype(BF16)
        out_copy(b).start()
    for b in range(rows):
        out_copy(b).wait()


def solution(mesh):
    seq = mesh.shape["seq"]

    def shard_body(tok, lens, params, scale, w_in, w_out):
        rows, toks, width = tok.shape
        slots = params.shape[1]
        experts, _, ff = w_in.shape
        own = slots // seq
        chips = seq // CORES
        groups = rows // GROUP_ROWS
        far = chips // 2
        hs = own // HALVES
        par = slots // CORES
        count = rows * own
        dims = (rows, toks, width, slots, seq, experts)
        dma = pltpu.SemaphoreType.DMA
        any_spec = pl.BlockSpec(memory_space=pl.ANY)
        vmem = pl.BlockSpec(memory_space=pltpu.VMEM)
        comb, gat, reach = pl.pallas_call(
            functools.partial(_exchange_kernel, dims),
            out_shape=(pltpu.VMEM((rows, toks, slots), BF16),
                       pltpu.VMEM((rows, HALVES, seq, hs, width), BF16),
                       pltpu.VMEM((rows, 128), jnp.int32)),
            in_specs=[any_spec, pl.BlockSpec(memory_space=pltpu.SMEM)] + [any_spec] * 4,
            out_specs=(vmem, vmem, vmem),
            scratch_shapes=[
                pltpu.SMEM((rows,), jnp.int32),
                pltpu.VMEM((rows, toks, width), BF16),
                pltpu.VMEM((rows, toks, width), BF16),
                pltpu.VMEM((width, slots), BF16),
                pltpu.VMEM((slots, width), BF16),
                pltpu.VMEM((slots, width), BF16),
                pltpu.VMEM((CORES, rows, HALVES, chips, hs, width), BF16),
                pltpu.VMEM((rows, HALVES, chips, hs, width), BF16),
                pltpu.VMEM((rows, HALVES, chips, hs, width), BF16),
                pltpu.VMEM((2, HALVES, rows, hs, width), BF16),
                pltpu.VMEM((2, 4, HALVES, rows, hs, width), BF16),
                pltpu.VMEM((CORES, par, 128), F32),
                pltpu.VMEM((par, 128), F32),
                pltpu.VMEM((HALVES, chips, hs, 128), BF16),
                pltpu.VMEM((chips, HALVES, hs, 128), BF16),
                pltpu.VMEM((HALVES, rows, hs, width), F32),
                pltpu.VMEM((HALVES, count // HALVES, width), BF16),
                pltpu.VMEM((experts, width, ff), BF16),
                pltpu.VMEM((experts, ff, width), BF16),
                pltpu.VMEM((count // HALVES, width), BF16),
                pltpu.VMEM((2, slots, toks), BF16),
                dma((4,)), dma, dma, dma((HALVES,)), dma, dma((groups,)), dma((2,)), dma((2,)),
                dma((2, groups, HALVES)), dma((HALVES,)), dma,
                dma((HALVES, CHUNKS, 4)), dma, dma((CHUNKS,)),
            ],
            compiler_params=pltpu.CompilerParams(
                collective_id=0, has_side_effects=True, vmem_limit_bytes=VMEM_LIMIT),
            name="exchange",
        )(lens, scale, params, tok, w_in, w_out)
        gat = gat.reshape(rows, slots, width)
        return pl.pallas_call(
            _combine_kernel,
            out_shape=jax.ShapeDtypeStruct((rows, toks, width), BF16),
            in_specs=[vmem, vmem, vmem],
            out_specs=any_spec,
            scratch_shapes=[pltpu.VMEM((rows, toks, width), BF16), dma((rows,))],
            compiler_params=pltpu.CompilerParams(vmem_limit_bytes=COMBINE_LIMIT),
            name="combine",
        )(reach, comb, gat)

    return jax.shard_map(
        shard_body,
        mesh=mesh,
        in_specs=(P("data", "seq", None), P("data"), P(None, None), P(None), P("seq", None, None), P("seq", None, None)),
        out_specs=P("data", "seq", None),
        check_vma=False,
    )
```

```python
import functools

import jax
import jax.numpy as jnp
from jax import lax
from jax.experimental import pallas as pl
from jax.experimental.pallas import tpu as pltpu
from jax.sharding import PartitionSpec as P

F32 = jnp.float32
BF16 = jnp.bfloat16
MESH = pl.DeviceIdType.MESH
NT = (((1,), (1,)), ((), ()))
UP, DOWN = 0, 1
GROUP_ROWS = 2
HALVES = 2
CORES = 2
CHUNKS = 2
ORDER = (
    ("disp", 0), ("disp", 1), ("disp", 2), ("bar",), ("pair", 0), ("disp", 3), ("disp", 4), ("total", 0),
    ("pair", 1), ("first", 0, 0), ("disp", 5), ("first", 0, 1), ("disp", 6), ("total", 1), ("first", 1, 1),
    ("pair", 2), ("first", 1, 0), ("disp", 7), ("disp", 8), ("total", 2), ("pair", 3), ("zpair",),
    ("first", 2, 0), ("relay", 0, 0), ("comb", 0), ("total", 3), ("first", 3, 0), ("first", 3, 1), ("z",),
    ("first", 2, 1), ("comb", 1), ("relay", 1, 0), ("comb", 2), ("relay", 2, 0), ("comb", 3), ("relay", 3, 0),
    ("comb", 4), ("comb", 5), ("relay", 0, 1), ("comb", 6), ("relay", 1, 1), ("relay", 2, 1), ("relay", 3, 1),
    ("fin", 0), ("ffn", 0), ("dfar", 0, 0), ("dfar", 0, 1), ("dnear", 0, 0), ("dnear", 0, 1), ("fin", 1),
    ("ffn", 1), ("dfar", 1, 0), ("dfar", 1, 1), ("fwd", 0, 0), ("fwd", 0, 1), ("dnear", 1, 0), ("dnear", 1, 1),
    ("near", 0, 0), ("near", 0, 1), ("fwd", 1, 0), ("fwd", 1, 1), ("coll", 0, 0), ("coll", 0, 1),
    ("near", 1, 0), ("near", 1, 1), ("comb", 7), ("coll", 1, 0), ("coll", 1, 1),
)
PARTS = 2
TAIL = 4
VMEM_LIMIT = 52 * 1024 * 1024
COMBINE_LIMIT = 20 * 1024 * 1024


def _exchange_kernel(dims, len_hbm, scale_ref, phi_ref, tok_ref, win_ref, wout_ref, comb_ref, gat_ref, lens_ref,
                     len_ref, xbuf, xnbuf, phi_in, phi_ring, phi_comb, part, pin, chip, cbuf, rbuf, zpart, zpin, zchip, zrecv,
                     slot_in, by_expert, win, wout, ypart, wbuf,
                     x_sem, phi_sem, scalar_sem, w_sem, pr_send, pr_recv, zp_sem, z_sem, relay_recv, fin_recv, rs_send,
                     ag_recv, ag_send, pg_recv):
    rows, toks, width, slots, seq, experts = dims
    chips = seq // CORES
    own = slots // seq
    per = own // experts
    groups = rows // GROUP_ROWS
    far = chips // 2
    half_e = experts // HALVES
    hs = own // HALVES
    par = slots // CORES

    me = lax.axis_index("seq")
    z = me // CORES
    core = me % CORES
    other = 1 - core
    partner = z * CORES + other

    def chip_at(delta):
        return (z + delta + chips) % chips

    def dev_at(delta):
        return chip_at(delta) * CORES + core

    def sign(way):
        return 1 if way == UP else -1

    def remote(src, dst, send, recv, dev):
        return pltpu.make_async_remote_copy(
            src_ref=src, dst_ref=dst, send_sem=send, recv_sem=recv, device_id={"seq": dev}, device_id_type=MESH)

    def wait_bytes(ref, sem):
        pltpu.make_async_copy(ref, ref, sem).wait()

    x_parts = {0: pl.ds(0, 1), 1: pl.ds(1, 1), 2: pl.ds(2, 2), 4: pl.ds(4, rows - 4)}
    x_copies = {b: pltpu.make_async_copy(tok_ref.at[p], xbuf.at[p], x_sem.at[i]) for i, (b, p) in enumerate(x_parts.items())}
    phi_copy = pltpu.make_async_copy(phi_ref, phi_in, phi_sem)
    len_copy = pltpu.make_async_copy(len_hbm, len_ref, scalar_sem)
    phi_copy.start()
    len_copy.start()
    x_copies[0].start()
    x_copies[1].start()

    barrier = pltpu.get_barrier_semaphore()
    for delta in range(1, chips):
        pl.semaphore_signal(barrier, inc=1, device_id={"seq": dev_at(delta)}, device_id_type=MESH)
    pl.semaphore_signal(barrier, inc=1, device_id={"seq": partner}, device_id_type=MESH)

    n0 = lax.broadcasted_iota(jnp.int32, (slots, slots), 0)
    n1 = lax.broadcasted_iota(jnp.int32, (slots, slots), 1)
    ring_src = ((n0 % (par // HALVES)) // hs * CORES + n0 // par) * own + (n0 % par) // (par // HALVES) * hs + n0 % hs
    comb_src = (n0 % (seq * hs)) // hs * own + n0 // (seq * hs) * hs + n0 % hs
    ring_hot = jnp.where(n1 == ring_src, 1.0, 0.0).astype(BF16)
    comb_hot = jnp.where(n1 == comb_src, 1.0, 0.0).astype(BF16)
    with jax.named_scope("phiwait"):
        phi_copy.wait()
        len_copy.wait()
    gain = scale_ref[0]
    x_copies[2].start()
    x_copies[4].start()
    params = phi_in[...].astype(F32)
    col_inv = lax.rsqrt(jnp.sum(params * params, axis=0, keepdims=True) + 1e-6)
    phi_norm = (params * (gain * col_inv)).astype(BF16)
    phi_ring[...] = lax.dot_general(ring_hot, phi_norm, NT, preferred_element_type=F32).astype(BF16)
    phi_comb[...] = lax.dot_general(comb_hot, phi_norm, NT, preferred_element_type=F32).astype(BF16)
    bound = gain * 1.01
    zlane = lax.broadcasted_iota(jnp.int32, (slots, 128), 1)
    zpart[...] = jnp.zeros_like(zpart)
    row_id = lax.broadcasted_iota(jnp.int32, lens_ref.shape, 0)
    lens = jnp.zeros(lens_ref.shape, jnp.int32)
    for b in range(rows):
        lens = jnp.where(row_id == b, len_ref[b], lens)
    lens_ref[...] = lens

    def normalize_part(b, ts):
        xf = xbuf[b, ts].astype(F32)
        inv = lax.rsqrt(jnp.sum(xf * xf, axis=-1, keepdims=True) + 1e-6)
        xnbuf[b, ts] = (xf * inv).astype(BF16)

    def weigh(r, ts):
        lt = lax.dot_general(phi_ring[...], xnbuf[r, ts], NT, preferred_element_type=F32)
        pos = me * toks + ts.start + lax.broadcasted_iota(jnp.int32, (1, ts.size), 1)
        w = jnp.exp(lt - jnp.where(pos < len_ref[r], bound, 1e30))
        wbuf[r % 2, :, ts] = w.astype(BF16)
        return sum(w[:, i * 128:(i + 1) * 128] for i in range(ts.size // 128))

    def slot_sums(r, lo, hi):
        s = jnp.dot(wbuf[r % 2], xbuf[r, :, lo:hi], preferred_element_type=F32).astype(BF16)
        for p in range(CORES):
            part[p, r, :, :, :, lo:hi] = s[p * par:(p + 1) * par].reshape(HALVES, chips, hs, hi - lo)

    def dispatch_stage(r):
        tile = toks // PARTS
        zs = jnp.zeros((slots, 128), F32)
        if r >= 1:
            slot_sums(r - 1, 0, width)
        for c in range(PARTS):
            ts = pl.ds(c * tile, tile)
            if r < rows:
                zs = zs + weigh(r, ts)
            if r + 1 < rows:
                normalize_part(r + 1, ts)
        if r < rows:
            zsum = jnp.sum(zs, axis=1, keepdims=True)
            hit = jnp.where(zlane == r, zsum, zpart[...].reshape(slots, 128))
            zpart[...] = hit.reshape(CORES, par, 128)

    def combine_row(b):
        logits = lax.dot_general(xnbuf[b], phi_comb[...], NT, preferred_element_type=F32)
        e = jnp.exp(logits)
        total = jnp.sum(e, axis=-1, keepdims=True)
        comb_ref[b] = (e * (1.0 / total)).astype(BF16)

    def span(g):
        return pl.ds(g * GROUP_ROWS, GROUP_ROWS)

    def pair_copy(g):
        return remote(part.at[other, span(g)], pin.at[span(g)], pr_send, pr_recv.at[g], partner)

    def zpair_copy():
        return remote(zpart.at[other], zpin, zp_sem.at[0], zp_sem.at[1], partner)

    def chip_sum(g):
        pair_copy(g).wait_recv()
        chip[span(g)] = (part[core, span(g)].astype(F32) + pin[span(g)].astype(F32)).astype(BF16)

    def is_far(way, index):
        return (index % 2 == 0) == (way == UP)

    def rs_first(g, h):
        for way in (UP, DOWN):
            s = sign(way)
            relay = relay_recv.at[way, g, h]
            if is_far(way, g + h):
                remote(chip.at[span(g), h, chip_at(far * s)], rbuf.at[way, 0, h, span(g)], rs_send, relay, dev_at(2 * s)).start()
            remote(chip.at[span(g), h, chip_at(3 * s)], rbuf.at[way, 1, h, span(g)], rs_send, relay, dev_at(s)).start()
        for way in (UP, DOWN):
            s = sign(way)
            remote(chip.at[span(g), h, chip_at(s)], rbuf.at[way, 3, h, span(g)], rs_send, fin_recv.at[h], dev_at(s)).start()

    def rs_relay(g, h):
        for way in (UP, DOWN):
            s = sign(way)
            first = 0 if is_far(way, g + h) else 1
            with jax.named_scope(f"relay{g}_{h}_{way}"):
                wait_bytes(rbuf.at[way, pl.ds(first, 2 - first), h, span(g)], relay_recv.at[way, g, h])
            total = chip[span(g), h, chip_at(2 * s)].astype(F32)
            for kind in range(first, 2):
                total = total + rbuf[way, kind, h, span(g)].astype(F32)
            cbuf[way, h, span(g)] = total.astype(BF16)
            remote(cbuf.at[way, h, span(g)], rbuf.at[way, 2, h, span(g)], rs_send, fin_recv.at[h], dev_at(2 * s)).start()

    def z_exchange():
        zpair_copy().wait_recv()
        zs = zpart[core] + zpin[...]
        zl = lax.broadcasted_iota(jnp.int32, zs.shape, 1)
        hi = zs.astype(BF16).astype(F32)
        mid = (zs - hi).astype(BF16).astype(F32)
        low = zs - hi - mid
        split = jnp.where(zl < rows, hi, 0.0)
        split = split + jnp.where((zl >= rows) & (zl < 2 * rows), pltpu.roll(mid, rows, 1), 0.0)
        split = split + jnp.where((zl >= 2 * rows) & (zl < 3 * rows), pltpu.roll(low, 2 * rows, 1), 0.0)
        zchip[...] = split.astype(BF16).reshape(zchip.shape)
        for delta in range(1, chips):
            remote(zchip.at[:, chip_at(delta)], zrecv.at[delta], z_sem.at[0], z_sem.at[1], dev_at(delta)).start()

    def weights(h):
        es = pl.ds(h * half_e, half_e)
        return (pltpu.make_async_copy(win_ref.at[es], win.at[es], w_sem.at[h]),
                pltpu.make_async_copy(wout_ref.at[es], wout.at[es], w_sem.at[h]))

    def disp(b):
        if b + 1 in x_parts:
            with jax.named_scope(f"x{b + 1}"):
                x_copies[b + 1].wait()
        with jax.named_scope(f"disp{b}"):
            dispatch_stage(b)
        if b == 1:
            for h in range(HALVES):
                for copy in weights(h):
                    copy.start()

    def comb(b):
        with jax.named_scope(f"comb{b}"):
            combine_row(b)

    def total(g):
        with jax.named_scope(f"sum{g}"):
            chip_sum(g)

    def greet():
        with jax.named_scope("barrier"):
            pl.semaphore_wait(barrier, chips)

    rb = rows * per
    hc = half_e * rb
    j0 = lax.broadcasted_iota(jnp.int32, (hc, hc), 0)
    j1 = lax.broadcasted_iota(jnp.int32, (hc, hc), 1)
    back = ((j0 % hs) // per) * rb + (j0 // hs) * per + j0 % per
    unperm = jnp.where(j1 == back, 1.0, 0.0).astype(BF16)
    src = ((j0 % rb) // per) * hs + (j0 // rb) * per + j0 % per
    perm = jnp.where(j1 == src, 1.0, 0.0).astype(BF16)

    def own_inputs(h):
        if h == 0:
            with jax.named_scope("zwait"):
                wait_bytes(zrecv.at[pl.ds(1, chips - 1)], z_sem.at[1])
        zsum = zchip[h, z].astype(F32)
        for delta in range(1, chips):
            zsum = zsum + zrecv[delta, h].astype(F32)
        lane = lax.broadcasted_iota(jnp.int32, zsum.shape, 1)
        zrow = []
        for b in range(rows):
            mine = (lane % rows == b) & (lane < 3 * rows)
            zrow.append(jnp.sum(jnp.where(mine, zsum, 0.0), axis=-1, keepdims=True))
        with jax.named_scope(f"fin{h}"):
            wait_bytes(rbuf.at[:, pl.ds(2, 2), h], fin_recv.at[h])
        for b in range(rows):
            s = chip[b, h, z].astype(F32)
            for way in (UP, DOWN):
                s = s + (rbuf[way, 2, h, b].astype(F32) + rbuf[way, 3, h, b].astype(F32))
            slot_in[h, b] = s / zrow[b]
        inputs = slot_in[h].reshape(rows * hs, width).astype(BF16)
        by_expert[h] = jnp.dot(perm, inputs, preferred_element_type=F32).astype(BF16)

    crows = rows // CHUNKS

    def chunk(c):
        return pl.ds(c * crows, crows)

    def send(h, c, delta, sem, to):
        ref = gat_ref.at[chunk(c), h, dev_at(delta)]
        remote(ref, ref, ag_send, ag_recv.at[h, c, sem], dev_at(to)).start()

    def arrived(h, c, sem, count):
        with jax.named_scope(f"ag_h{h}_c{c}_s{sem}"):
            wait_bytes(gat_ref.at[chunk(c), h, pl.ds(0, count)], ag_recv.at[h, c, sem])

    def publish(h, c, delta):
        ref = gat_ref.at[chunk(c), h, dev_at(delta)]
        remote(ref, ref, ag_send, pg_recv.at[c], partner).start()

    def direct_far(h, c):
        for way in (UP, DOWN):
            send(h, c, 0, way, 2 * sign(way))

    def direct_near(h, c):
        for way in (UP, DOWN):
            send(h, c, 0, 2, sign(way))
        publish(h, c, 0)

    def forward(h, c):
        for way in (UP, DOWN):
            s = sign(way)
            arrived(h, c, way, 1)
            if is_far(way, c):
                send(h, c, -2 * s, 3, 2 * s)
            send(h, c, -2 * s, 3, s)
            publish(h, c, -2 * s)

    def near(h, c):
        arrived(h, c, 2, 2)
        publish(h, c, -1)
        publish(h, c, 1)

    def collect(h, c):
        arrived(h, c, 3, 3)
        publish(h, c, -3)
        publish(h, c, 3)
        publish(h, c, -far if is_far(UP, c) else far)

    def expert_half(h):
        with jax.named_scope(f"wwait{h}"):
            wait_bytes(win, w_sem.at[h])
        with jax.named_scope(f"ffn{h}"):
            for i in range(half_e):
                e = h * half_e + i
                hid = jnp.dot(by_expert[h, i * rb:(i + 1) * rb], win[e], preferred_element_type=F32)
                hid = jax.nn.gelu(hid).astype(BF16)
                ypart[i * rb:(i + 1) * rb] = jnp.dot(hid, wout[e], preferred_element_type=F32).astype(BF16)
            blk = jnp.dot(unperm, ypart[...], preferred_element_type=F32)
            gat_ref[:, h, me] = blk.reshape(rows, hs, width).astype(BF16)

    events = {
        "disp": disp, "bar": greet, "pair": lambda g: pair_copy(g).start(), "total": total, "first": rs_first,
        "relay": rs_relay, "zpair": lambda: zpair_copy().start(), "z": z_exchange, "comb": comb, "fin": own_inputs,
        "ffn": expert_half, "dfar": direct_far, "dnear": direct_near, "fwd": forward, "near": near,
        "coll": collect,
    }
    with jax.named_scope("x0"):
        x_copies[0].wait()
    with jax.named_scope("norm0"):
        normalize_part(0, pl.ds(0, toks))
    for event in ORDER:
        events[event[0]](*event[1:])

    with jax.named_scope("end"):
        for c in range(CHUNKS):
            wait_bytes(gat_ref.at[chunk(c), :, pl.ds(0, chips)], pg_recv.at[c])
        wait_bytes(gat_ref.at[:, :, pl.ds(0, seq - 1)], ag_send)
        wait_bytes(pin, pr_send)
        zpair_copy().wait_send()
        wait_bytes(zrecv.at[pl.ds(1, chips - 1)], z_sem.at[0])
        wait_bytes(part.at[0, :, :, pl.ds(0, chips - 1)], rs_send)


def _combine_kernel(reach_ref, comb_ref, gat_ref, out_ref, ybuf, y_sem):
    rows, toks, width = ybuf.shape
    lanes = reach_ref.shape[1]
    pos = lax.axis_index("seq") * toks + lax.broadcasted_iota(jnp.int32, (toks, lanes), 0)

    pieces = [(b, 0, toks) for b in range(rows - 1)]
    size = toks // TAIL
    pieces += [(rows - 1, k * size, size) for k in range(TAIL)]
    copies = []
    for n, (b, first, size) in enumerate(pieces):
        ts = pl.ds(first, size)
        acc = jnp.dot(comb_ref[b, ts], gat_ref[b], preferred_element_type=F32)
        valid = pos[first:first + size] < reach_ref[b:b + 1]
        for i in range(width // lanes):
            part = slice(i * lanes, (i + 1) * lanes)
            ybuf[b, ts, part] = jnp.where(valid, acc[:, part], 0.0).astype(BF16)
        copies.append(pltpu.make_async_copy(ybuf.at[b, ts], out_ref.at[b, ts], y_sem.at[n]))
        copies[-1].start()
    for copy in copies:
        copy.wait()


def solution(mesh):
    seq = mesh.shape["seq"]

    def shard_body(tok, lens, params, scale, w_in, w_out):
        rows, toks, width = tok.shape
        slots = params.shape[1]
        experts, _, ff = w_in.shape
        own = slots // seq
        chips = seq // CORES
        groups = rows // GROUP_ROWS
        far = chips // 2
        hs = own // HALVES
        par = slots // CORES
        count = rows * own
        dims = (rows, toks, width, slots, seq, experts)
        dma = pltpu.SemaphoreType.DMA
        any_spec = pl.BlockSpec(memory_space=pl.ANY)
        vmem = pl.BlockSpec(memory_space=pltpu.VMEM)
        comb, gat, reach = pl.pallas_call(
            functools.partial(_exchange_kernel, dims),
            out_shape=(pltpu.VMEM((rows, toks, slots), BF16),
                       pltpu.VMEM((rows, HALVES, seq, hs, width), BF16),
                       pltpu.VMEM((rows, 128), jnp.int32)),
            in_specs=[any_spec, pl.BlockSpec(memory_space=pltpu.SMEM)] + [any_spec] * 4,
            out_specs=(vmem, vmem, vmem),
            scratch_shapes=[
                pltpu.SMEM((rows,), jnp.int32),
                pltpu.VMEM((rows, toks, width), BF16),
                pltpu.VMEM((rows, toks, width), BF16),
                pltpu.VMEM((width, slots), BF16),
                pltpu.VMEM((slots, width), BF16),
                pltpu.VMEM((slots, width), BF16),
                pltpu.VMEM((CORES, rows, HALVES, chips, hs, width), BF16),
                pltpu.VMEM((rows, HALVES, chips, hs, width), BF16),
                pltpu.VMEM((rows, HALVES, chips, hs, width), BF16),
                pltpu.VMEM((2, HALVES, rows, hs, width), BF16),
                pltpu.VMEM((2, 4, HALVES, rows, hs, width), BF16),
                pltpu.VMEM((CORES, par, 128), F32),
                pltpu.VMEM((par, 128), F32),
                pltpu.VMEM((HALVES, chips, hs, 128), BF16),
                pltpu.VMEM((chips, HALVES, hs, 128), BF16),
                pltpu.VMEM((HALVES, rows, hs, width), F32),
                pltpu.VMEM((HALVES, count // HALVES, width), BF16),
                pltpu.VMEM((experts, width, ff), BF16),
                pltpu.VMEM((experts, ff, width), BF16),
                pltpu.VMEM((count // HALVES, width), BF16),
                pltpu.VMEM((2, slots, toks), BF16),
                dma((4,)), dma, dma, dma((HALVES,)), dma, dma((groups,)), dma((2,)), dma((2,)),
                dma((2, groups, HALVES)), dma((HALVES,)), dma,
                dma((HALVES, CHUNKS, 4)), dma, dma((CHUNKS,)),
            ],
            compiler_params=pltpu.CompilerParams(
                collective_id=0, has_side_effects=True, vmem_limit_bytes=VMEM_LIMIT),
            name="exchange",
        )(lens, scale, params, tok, w_in, w_out)
        gat = gat.reshape(rows, slots, width)
        return pl.pallas_call(
            _combine_kernel,
            out_shape=jax.ShapeDtypeStruct((rows, toks, width), BF16),
            in_specs=[vmem, vmem, vmem],
            out_specs=any_spec,
            scratch_shapes=[pltpu.VMEM((rows, toks, width), BF16), dma((rows - 1 + TAIL,))],
            compiler_params=pltpu.CompilerParams(vmem_limit_bytes=COMBINE_LIMIT),
            name="combine",
        )(reach, comb, gat)

    return jax.shard_map(
        shard_body,
        mesh=mesh,
        in_specs=(P("data", "seq", None), P("data"), P(None, None), P(None), P("seq", None, None), P("seq", None, None)),
        out_specs=P("data", "seq", None),
        check_vma=False,
    )
```

```python
import functools

import jax
import jax.numpy as jnp
from jax import lax
from jax.experimental import pallas as pl
from jax.experimental.pallas import tpu as pltpu
from jax.sharding import PartitionSpec as P

F32 = jnp.float32
BF16 = jnp.bfloat16
MESH = pl.DeviceIdType.MESH
NT = (((1,), (1,)), ((), ()))
UP, DOWN = 0, 1
GROUP_ROWS = 2
HALVES = 2
CORES = 2
CHUNKS = 2
ORDER = (
    ("disp", 0), ("disp", 1), ("disp", 2), ("bar",), ("pair", 0), ("disp", 3), ("disp", 4), ("total", 0),
    ("pair", 1), ("first", 0, 0), ("disp", 5), ("first", 0, 1), ("disp", 6), ("total", 1), ("first", 1, 1),
    ("pair", 2), ("first", 1, 0), ("disp", 7), ("disp", 8), ("total", 2), ("pair", 3), ("zpair",),
    ("first", 2, 0), ("relay", 0, 0), ("comb", 0), ("total", 3), ("first", 3, 0), ("first", 3, 1), ("z",),
    ("first", 2, 1), ("comb", 1), ("relay", 1, 0), ("comb", 2), ("relay", 2, 0), ("comb", 3), ("relay", 3, 0),
    ("comb", 4), ("comb", 5), ("relay", 0, 1), ("comb", 6), ("relay", 1, 1), ("relay", 2, 1), ("relay", 3, 1),
    ("fin", 0), ("ffn", 0), ("dfar", 0, 0), ("dfar", 0, 1), ("dnear", 0, 0), ("dnear", 0, 1), ("fin", 1),
    ("ffn", 1), ("dfar", 1, 0), ("dfar", 1, 1), ("fwd", 0, 0), ("fwd", 0, 1), ("dnear", 1, 0), ("dnear", 1, 1),
    ("near", 0, 0), ("near", 0, 1), ("fwd", 1, 0), ("fwd", 1, 1), ("comb", 7), ("coll", 0, 0), ("coll", 0, 1),
    ("near", 1, 0), ("near", 1, 1), ("coll", 1, 0), ("coll", 1, 1),
)
PARTS = 2
TAIL = 4
VMEM_LIMIT = 52 * 1024 * 1024
COMBINE_LIMIT = 20 * 1024 * 1024


def _exchange_kernel(dims, len_hbm, scale_ref, phi_ref, tok_ref, win_ref, wout_ref, comb_ref, gat_ref, lens_ref,
                     len_ref, xbuf, xnbuf, phi_in, phi_ring, phi_comb, part, pin, chip, cbuf, rbuf, zpart, zpin, zchip, zrecv,
                     slot_in, by_expert, win, wout, ypart, wbuf,
                     x_sem, phi_sem, scalar_sem, w_sem, pr_send, pr_recv, zp_sem, z_sem, relay_recv, fin_recv, rs_send,
                     ag_recv, ag_send, pg_recv):
    rows, toks, width, slots, seq, experts = dims
    chips = seq // CORES
    own = slots // seq
    per = own // experts
    groups = rows // GROUP_ROWS
    far = chips // 2
    half_e = experts // HALVES
    hs = own // HALVES
    par = slots // CORES

    me = lax.axis_index("seq")
    z = me // CORES
    core = me % CORES
    other = 1 - core
    partner = z * CORES + other

    def chip_at(delta):
        return (z + delta + chips) % chips

    def dev_at(delta):
        return chip_at(delta) * CORES + core

    def sign(way):
        return 1 if way == UP else -1

    def remote(src, dst, send, recv, dev):
        return pltpu.make_async_remote_copy(
            src_ref=src, dst_ref=dst, send_sem=send, recv_sem=recv, device_id={"seq": dev}, device_id_type=MESH)

    def wait_bytes(ref, sem):
        pltpu.make_async_copy(ref, ref, sem).wait()

    x_parts = {0: pl.ds(0, 1), 1: pl.ds(1, 1), 2: pl.ds(2, 2), 4: pl.ds(4, rows - 4)}
    x_copies = {b: pltpu.make_async_copy(tok_ref.at[p], xbuf.at[p], x_sem.at[i]) for i, (b, p) in enumerate(x_parts.items())}
    phi_copy = pltpu.make_async_copy(phi_ref, phi_in, phi_sem)
    len_copy = pltpu.make_async_copy(len_hbm, len_ref, scalar_sem)
    phi_copy.start()
    len_copy.start()
    x_copies[0].start()
    x_copies[1].start()

    barrier = pltpu.get_barrier_semaphore()
    for delta in range(1, chips):
        pl.semaphore_signal(barrier, inc=1, device_id={"seq": dev_at(delta)}, device_id_type=MESH)
    pl.semaphore_signal(barrier, inc=1, device_id={"seq": partner}, device_id_type=MESH)

    n0 = lax.broadcasted_iota(jnp.int32, (slots, slots), 0)
    n1 = lax.broadcasted_iota(jnp.int32, (slots, slots), 1)
    ring_src = ((n0 % (par // HALVES)) // hs * CORES + n0 // par) * own + (n0 % par) // (par // HALVES) * hs + n0 % hs
    comb_src = (n0 % (seq * hs)) // hs * own + n0 // (seq * hs) * hs + n0 % hs
    ring_hot = jnp.where(n1 == ring_src, 1.0, 0.0).astype(BF16)
    comb_hot = jnp.where(n1 == comb_src, 1.0, 0.0).astype(BF16)
    with jax.named_scope("phiwait"):
        phi_copy.wait()
        len_copy.wait()
    gain = scale_ref[0]
    x_copies[2].start()
    x_copies[4].start()
    params = phi_in[...].astype(F32)
    col_inv = lax.rsqrt(jnp.sum(params * params, axis=0, keepdims=True) + 1e-6)
    phi_norm = (params * (gain * col_inv)).astype(BF16)
    phi_ring[...] = lax.dot_general(ring_hot, phi_norm, NT, preferred_element_type=F32).astype(BF16)
    phi_comb[...] = lax.dot_general(comb_hot, phi_norm, NT, preferred_element_type=F32).astype(BF16)
    bound = gain * 1.01
    zlane = lax.broadcasted_iota(jnp.int32, (slots, 128), 1)
    zpart[...] = jnp.zeros_like(zpart)
    row_id = lax.broadcasted_iota(jnp.int32, lens_ref.shape, 0)
    lens = jnp.zeros(lens_ref.shape, jnp.int32)
    for b in range(rows):
        lens = jnp.where(row_id == b, len_ref[b], lens)
    lens_ref[...] = lens

    def normalize_part(b, ts):
        xf = xbuf[b, ts].astype(F32)
        inv = lax.rsqrt(jnp.sum(xf * xf, axis=-1, keepdims=True) + 1e-6)
        xnbuf[b, ts] = (xf * inv).astype(BF16)

    def weigh(r, ts):
        lt = lax.dot_general(phi_ring[...], xnbuf[r, ts], NT, preferred_element_type=F32)
        pos = me * toks + ts.start + lax.broadcasted_iota(jnp.int32, (1, ts.size), 1)
        w = jnp.exp(lt - jnp.where(pos < len_ref[r], bound, 1e30))
        wbuf[r % 2, :, ts] = w.astype(BF16)
        return sum(w[:, i * 128:(i + 1) * 128] for i in range(ts.size // 128))

    def slot_sums(r, lo, hi):
        s = jnp.dot(wbuf[r % 2], xbuf[r, :, lo:hi], preferred_element_type=F32).astype(BF16)
        for p in range(CORES):
            part[p, r, :, :, :, lo:hi] = s[p * par:(p + 1) * par].reshape(HALVES, chips, hs, hi - lo)

    def dispatch_stage(r):
        tile = toks // PARTS
        zs = jnp.zeros((slots, 128), F32)
        if r >= 1:
            slot_sums(r - 1, 0, width)
        for c in range(PARTS):
            ts = pl.ds(c * tile, tile)
            if r < rows:
                zs = zs + weigh(r, ts)
            if r + 1 < rows:
                normalize_part(r + 1, ts)
        if r < rows:
            zsum = jnp.sum(zs, axis=1, keepdims=True)
            hit = jnp.where(zlane == r, zsum, zpart[...].reshape(slots, 128))
            zpart[...] = hit.reshape(CORES, par, 128)

    def combine_row(b):
        logits = lax.dot_general(xnbuf[b], phi_comb[...], NT, preferred_element_type=F32)
        e = jnp.exp(logits)
        total = jnp.sum(e, axis=-1, keepdims=True)
        comb_ref[b] = (e * (1.0 / total)).astype(BF16)

    def span(g):
        return pl.ds(g * GROUP_ROWS, GROUP_ROWS)

    def pair_copy(g):
        return remote(part.at[other, span(g)], pin.at[span(g)], pr_send, pr_recv.at[g], partner)

    def zpair_copy():
        return remote(zpart.at[other], zpin, zp_sem.at[0], zp_sem.at[1], partner)

    def chip_sum(g):
        pair_copy(g).wait_recv()
        chip[span(g)] = (part[core, span(g)].astype(F32) + pin[span(g)].astype(F32)).astype(BF16)

    def is_far(way, index):
        return (index % 2 == 0) == (way == UP)

    def rs_first(g, h):
        for way in (UP, DOWN):
            s = sign(way)
            relay = relay_recv.at[way, g, h]
            if is_far(way, g + h):
                remote(chip.at[span(g), h, chip_at(far * s)], rbuf.at[way, 0, h, span(g)], rs_send, relay, dev_at(2 * s)).start()
            remote(chip.at[span(g), h, chip_at(3 * s)], rbuf.at[way, 1, h, span(g)], rs_send, relay, dev_at(s)).start()
        for way in (UP, DOWN):
            s = sign(way)
            remote(chip.at[span(g), h, chip_at(s)], rbuf.at[way, 3, h, span(g)], rs_send, fin_recv.at[h], dev_at(s)).start()

    def rs_relay(g, h):
        for way in (UP, DOWN):
            s = sign(way)
            first = 0 if is_far(way, g + h) else 1
            with jax.named_scope(f"relay{g}_{h}_{way}"):
                wait_bytes(rbuf.at[way, pl.ds(first, 2 - first), h, span(g)], relay_recv.at[way, g, h])
            total = chip[span(g), h, chip_at(2 * s)].astype(F32)
            for kind in range(first, 2):
                total = total + rbuf[way, kind, h, span(g)].astype(F32)
            cbuf[way, h, span(g)] = total.astype(BF16)
            remote(cbuf.at[way, h, span(g)], rbuf.at[way, 2, h, span(g)], rs_send, fin_recv.at[h], dev_at(2 * s)).start()

    def z_exchange():
        zpair_copy().wait_recv()
        zs = zpart[core] + zpin[...]
        zl = lax.broadcasted_iota(jnp.int32, zs.shape, 1)
        hi = zs.astype(BF16).astype(F32)
        mid = (zs - hi).astype(BF16).astype(F32)
        low = zs - hi - mid
        split = jnp.where(zl < rows, hi, 0.0)
        split = split + jnp.where((zl >= rows) & (zl < 2 * rows), pltpu.roll(mid, rows, 1), 0.0)
        split = split + jnp.where((zl >= 2 * rows) & (zl < 3 * rows), pltpu.roll(low, 2 * rows, 1), 0.0)
        zchip[...] = split.astype(BF16).reshape(zchip.shape)
        for delta in range(1, chips):
            remote(zchip.at[:, chip_at(delta)], zrecv.at[delta], z_sem.at[0], z_sem.at[1], dev_at(delta)).start()

    def weights(h):
        es = pl.ds(h * half_e, half_e)
        return (pltpu.make_async_copy(win_ref.at[es], win.at[es], w_sem.at[h]),
                pltpu.make_async_copy(wout_ref.at[es], wout.at[es], w_sem.at[h]))

    def disp(b):
        if b + 1 in x_parts:
            with jax.named_scope(f"x{b + 1}"):
                x_copies[b + 1].wait()
        with jax.named_scope(f"disp{b}"):
            dispatch_stage(b)
        if b == 1:
            for h in range(HALVES):
                for copy in weights(h):
                    copy.start()

    def comb(b):
        with jax.named_scope(f"comb{b}"):
            combine_row(b)

    def total(g):
        with jax.named_scope(f"sum{g}"):
            chip_sum(g)

    def greet():
        with jax.named_scope("barrier"):
            pl.semaphore_wait(barrier, chips)

    rb = rows * per
    hc = half_e * rb
    j0 = lax.broadcasted_iota(jnp.int32, (hc, hc), 0)
    j1 = lax.broadcasted_iota(jnp.int32, (hc, hc), 1)
    back = ((j0 % hs) // per) * rb + (j0 // hs) * per + j0 % per
    unperm = jnp.where(j1 == back, 1.0, 0.0).astype(BF16)
    src = ((j0 % rb) // per) * hs + (j0 // rb) * per + j0 % per
    perm = jnp.where(j1 == src, 1.0, 0.0).astype(BF16)

    def own_inputs(h):
        if h == 0:
            with jax.named_scope("zwait"):
                wait_bytes(zrecv.at[pl.ds(1, chips - 1)], z_sem.at[1])
        zsum = zchip[h, z].astype(F32)
        for delta in range(1, chips):
            zsum = zsum + zrecv[delta, h].astype(F32)
        lane = lax.broadcasted_iota(jnp.int32, zsum.shape, 1)
        zrow = []
        for b in range(rows):
            mine = (lane % rows == b) & (lane < 3 * rows)
            zrow.append(jnp.sum(jnp.where(mine, zsum, 0.0), axis=-1, keepdims=True))
        with jax.named_scope(f"fin{h}"):
            wait_bytes(rbuf.at[:, pl.ds(2, 2), h], fin_recv.at[h])
        for b in range(rows):
            s = chip[b, h, z].astype(F32)
            for way in (UP, DOWN):
                s = s + (rbuf[way, 2, h, b].astype(F32) + rbuf[way, 3, h, b].astype(F32))
            slot_in[h, b] = s / zrow[b]
        inputs = slot_in[h].reshape(rows * hs, width).astype(BF16)
        by_expert[h] = jnp.dot(perm, inputs, preferred_element_type=F32).astype(BF16)

    crows = rows // CHUNKS

    def chunk(c):
        return pl.ds(c * crows, crows)

    def send(h, c, delta, sem, to):
        ref = gat_ref.at[chunk(c), h, dev_at(delta)]
        remote(ref, ref, ag_send, ag_recv.at[h, c, sem], dev_at(to)).start()

    def arrived(h, c, sem, count):
        with jax.named_scope(f"ag_h{h}_c{c}_s{sem}"):
            wait_bytes(gat_ref.at[chunk(c), h, pl.ds(0, count)], ag_recv.at[h, c, sem])

    def publish(h, c, delta):
        ref = gat_ref.at[chunk(c), h, dev_at(delta)]
        remote(ref, ref, ag_send, pg_recv.at[c], partner).start()

    def direct_far(h, c):
        for way in (UP, DOWN):
            send(h, c, 0, way, 2 * sign(way))

    def direct_near(h, c):
        for way in (UP, DOWN):
            send(h, c, 0, 2, sign(way))
        publish(h, c, 0)

    def forward(h, c):
        for way in (UP, DOWN):
            s = sign(way)
            arrived(h, c, way, 1)
            if is_far(way, c):
                send(h, c, -2 * s, 3, 2 * s)
            send(h, c, -2 * s, 3, s)
            publish(h, c, -2 * s)

    def near(h, c):
        arrived(h, c, 2, 2)
        publish(h, c, -1)
        publish(h, c, 1)

    def collect(h, c):
        arrived(h, c, 3, 3)
        publish(h, c, -3)
        publish(h, c, 3)
        publish(h, c, -far if is_far(UP, c) else far)

    def expert_half(h):
        with jax.named_scope(f"wwait{h}"):
            wait_bytes(win, w_sem.at[h])
        with jax.named_scope(f"ffn{h}"):
            for i in range(half_e):
                e = h * half_e + i
                hid = jnp.dot(by_expert[h, i * rb:(i + 1) * rb], win[e], preferred_element_type=F32)
                hid = jax.nn.gelu(hid).astype(BF16)
                ypart[i * rb:(i + 1) * rb] = jnp.dot(hid, wout[e], preferred_element_type=F32).astype(BF16)
            blk = jnp.dot(unperm, ypart[...], preferred_element_type=F32)
            gat_ref[:, h, me] = blk.reshape(rows, hs, width).astype(BF16)

    events = {
        "disp": disp, "bar": greet, "pair": lambda g: pair_copy(g).start(), "total": total, "first": rs_first,
        "relay": rs_relay, "zpair": lambda: zpair_copy().start(), "z": z_exchange, "comb": comb, "fin": own_inputs,
        "ffn": expert_half, "dfar": direct_far, "dnear": direct_near, "fwd": forward, "near": near,
        "coll": collect,
    }
    with jax.named_scope("x0"):
        x_copies[0].wait()
    with jax.named_scope("norm0"):
        normalize_part(0, pl.ds(0, toks))
    for event in ORDER:
        events[event[0]](*event[1:])

    with jax.named_scope("end"):
        for c in range(CHUNKS):
            wait_bytes(gat_ref.at[chunk(c), :, pl.ds(0, chips)], pg_recv.at[c])
        wait_bytes(gat_ref.at[:, :, pl.ds(0, seq - 1)], ag_send)
        wait_bytes(pin, pr_send)
        zpair_copy().wait_send()
        wait_bytes(zrecv.at[pl.ds(1, chips - 1)], z_sem.at[0])
        wait_bytes(part.at[0, :, :, pl.ds(0, chips - 1)], rs_send)


def _combine_kernel(reach_ref, comb_ref, gat_ref, out_ref, ybuf, y_sem):
    rows, toks, width = ybuf.shape
    lanes = reach_ref.shape[1]
    pos = lax.axis_index("seq") * toks + lax.broadcasted_iota(jnp.int32, (toks, lanes), 0)

    pieces = [(b, 0, toks) for b in range(rows - 1)]
    size = toks // TAIL
    pieces += [(rows - 1, k * size, size) for k in range(TAIL)]
    copies = []
    for n, (b, first, size) in enumerate(pieces):
        ts = pl.ds(first, size)
        acc = jnp.dot(comb_ref[b, ts], gat_ref[b], preferred_element_type=F32)
        valid = pos[first:first + size] < reach_ref[b:b + 1]
        for i in range(width // lanes):
            part = slice(i * lanes, (i + 1) * lanes)
            ybuf[b, ts, part] = jnp.where(valid, acc[:, part], 0.0).astype(BF16)
        copies.append(pltpu.make_async_copy(ybuf.at[b, ts], out_ref.at[b, ts], y_sem.at[n]))
        copies[-1].start()
    for copy in copies:
        copy.wait()


def solution(mesh):
    seq = mesh.shape["seq"]

    def shard_body(tok, lens, params, scale, w_in, w_out):
        rows, toks, width = tok.shape
        slots = params.shape[1]
        experts, _, ff = w_in.shape
        own = slots // seq
        chips = seq // CORES
        groups = rows // GROUP_ROWS
        far = chips // 2
        hs = own // HALVES
        par = slots // CORES
        count = rows * own
        dims = (rows, toks, width, slots, seq, experts)
        dma = pltpu.SemaphoreType.DMA
        any_spec = pl.BlockSpec(memory_space=pl.ANY)
        vmem = pl.BlockSpec(memory_space=pltpu.VMEM)
        comb, gat, reach = pl.pallas_call(
            functools.partial(_exchange_kernel, dims),
            out_shape=(pltpu.VMEM((rows, toks, slots), BF16),
                       pltpu.VMEM((rows, HALVES, seq, hs, width), BF16),
                       pltpu.VMEM((rows, 128), jnp.int32)),
            in_specs=[any_spec, pl.BlockSpec(memory_space=pltpu.SMEM)] + [any_spec] * 4,
            out_specs=(vmem, vmem, vmem),
            scratch_shapes=[
                pltpu.SMEM((rows,), jnp.int32),
                pltpu.VMEM((rows, toks, width), BF16),
                pltpu.VMEM((rows, toks, width), BF16),
                pltpu.VMEM((width, slots), BF16),
                pltpu.VMEM((slots, width), BF16),
                pltpu.VMEM((slots, width), BF16),
                pltpu.VMEM((CORES, rows, HALVES, chips, hs, width), BF16),
                pltpu.VMEM((rows, HALVES, chips, hs, width), BF16),
                pltpu.VMEM((rows, HALVES, chips, hs, width), BF16),
                pltpu.VMEM((2, HALVES, rows, hs, width), BF16),
                pltpu.VMEM((2, 4, HALVES, rows, hs, width), BF16),
                pltpu.VMEM((CORES, par, 128), F32),
                pltpu.VMEM((par, 128), F32),
                pltpu.VMEM((HALVES, chips, hs, 128), BF16),
                pltpu.VMEM((chips, HALVES, hs, 128), BF16),
                pltpu.VMEM((HALVES, rows, hs, width), F32),
                pltpu.VMEM((HALVES, count // HALVES, width), BF16),
                pltpu.VMEM((experts, width, ff), BF16),
                pltpu.VMEM((experts, ff, width), BF16),
                pltpu.VMEM((count // HALVES, width), BF16),
                pltpu.VMEM((2, slots, toks), BF16),
                dma((4,)), dma, dma, dma((HALVES,)), dma, dma((groups,)), dma((2,)), dma((2,)),
                dma((2, groups, HALVES)), dma((HALVES,)), dma,
                dma((HALVES, CHUNKS, 4)), dma, dma((CHUNKS,)),
            ],
            compiler_params=pltpu.CompilerParams(
                collective_id=0, has_side_effects=True, vmem_limit_bytes=VMEM_LIMIT),
            name="exchange",
        )(lens, scale, params, tok, w_in, w_out)
        gat = gat.reshape(rows, slots, width)
        return pl.pallas_call(
            _combine_kernel,
            out_shape=jax.ShapeDtypeStruct((rows, toks, width), BF16),
            in_specs=[vmem, vmem, vmem],
            out_specs=any_spec,
            scratch_shapes=[pltpu.VMEM((rows, toks, width), BF16), dma((rows - 1 + TAIL,))],
            compiler_params=pltpu.CompilerParams(vmem_limit_bytes=COMBINE_LIMIT),
            name="combine",
        )(reach, comb, gat)

    return jax.shard_map(
        shard_body,
        mesh=mesh,
        in_specs=(P("data", "seq", None), P("data"), P(None, None), P(None), P("seq", None, None), P("seq", None, None)),
        out_specs=P("data", "seq", None),
        check_vma=False,
    )
```
